256 devices in a mesh: lb: 8 (over z), rb: 16 (over x, y), wa: 2 (over core).
Axes of the slice: x: 4, y: 4, z: 8, core: 2. Of those that a mesh axis runs over, the one named last changes fastest.
Arguments:
- initial_guess: bfloat16 [8192, 4, 128], P(('lb', 'rb')), may hold values from -6 to 6
- left_environment: bfloat16 [8, 8, 16, 64, 8192], P('wa', None, 'rb', None, 'lb'), may hold values from -12 to 12, as said below
- right_environment: bfloat16 [128, 8, 128], replicated, may hold values from -12 to 12, as said below
- operator_blocks: float32 [16, 4, 4], replicated, may hold values from -4 to 4
- operator_pairs: int32 [16, 2], replicated, may hold values from 0 to 7
Outputs:
- ritz_vector: float32 [8192, 4, 128], P(('lb', 'rb'))
- residual: float32 [8192, 4, 128], P(('lb', 'rb'))
The draws below stay inside these ranges and needn't reach their ends.
Inputs may be any that keep to these rules, and one draw needn't show every extreme that they name: `operator_pairs`: each row names the left and the right MPO index of one operator block; blocks with the same pair add. `left_environment`: for each MPO index the [8192, 8192] matrix is symmetric. `right_environment`: for each MPO index the matrix over the two right bond states is symmetric.
All inputs are finite; a program needn't handle non-finite values.
Results may differ from the reference program's by a relative error of at most 0.014.
Values may be sent and summed in bfloat16 or wider, within the bound.
A program may use at most 128 MiB of HBM per device.

```python
import jax
import jax.numpy as jnp
from jax import lax

DL = 8192
RB = 128
W = 8
NB = 16
ITERS = 3
SWEEPS = 8
S = 4
N_LB = 8
N_RB = 16


def draw_left_environment(key, part):
    noise_key = jax.random.fold_in(key, 11)
    scale_key = jax.random.fold_in(key, 12)
    noise = jax.random.normal(noise_key, (W, DL, DL), jnp.float32)
    symmetric = (noise + jnp.swapaxes(noise, 1, 2)) * (0.5 / jnp.sqrt(DL * 1.0))
    scales = jnp.exp(jax.random.uniform(scale_key, (W, DL), jnp.float32, 0.0, 2.0))
    positions = jnp.arange(DL, dtype=jnp.int32)
    symmetric = symmetric.at[:, positions, positions].add(scales)
    return symmetric.reshape(W, N_LB, N_RB, DL // (N_LB * N_RB), DL).astype(jnp.bfloat16)


def draw_right_environment(key, part):
    noise_key = jax.random.fold_in(key, 21)
    scale_key = jax.random.fold_in(key, 22)
    noise = jax.random.normal(noise_key, (RB, W, RB), jnp.float32)
    symmetric = (noise + jnp.transpose(noise, (2, 1, 0))) * (0.5 / jnp.sqrt(RB * 1.0))
    scales = jnp.exp(jax.random.uniform(scale_key, (W, RB), jnp.float32, 0.0, 2.0))
    symmetric = symmetric + jnp.eye(RB, dtype=jnp.float32)[:, None, :] * scales[None, :, :]
    return symmetric.astype(jnp.bfloat16)


def place_ends(entries, rng, least, top_value):
    shape = entries.shape
    place = [jax.random.randint(jax.random.fold_in(rng, axis), (), 0, shape[axis]) for axis in range(len(shape))]
    entries = entries.at[tuple(place)].set(least)
    longest = shape.index(max(shape))
    place[longest] = (place[longest] + 1) % shape[longest]
    return entries.at[tuple(place)].set(top_value)


def block_scale(key, dims, split, smallest, high):
    loudness, own = 1.0, jax.random.fold_in(key, 6)
    for axis_at, parts in split:
        draws = jnp.exp(jax.random.uniform(jax.random.fold_in(own, axis_at), (parts,), jnp.float32, smallest / len(split), high / len(split)))
        loudness = loudness * jnp.repeat(draws, dims[axis_at] // parts).reshape([-1 if axis == axis_at else 1 for axis in range(len(dims))])
    return loudness


def scatter_about(key, extent, deviation, reach, shards=(), kind=jnp.bfloat16):
    values = deviation * jax.random.normal(key, extent, jnp.float32)
    if shards:
        values = values * block_scale(key, extent, shards, -0.22, 0.18)
    return jnp.clip(values, -reach, reach).astype(kind)


def setup_inputs(seed: int = 0) -> dict:
    key_list = jax.random.split(jax.random.key(seed), 6)
    initial_guess = scatter_about(key_list[0], (DL, S, RB), 1.0, 6.0, ((0, 128),))
    left_environment = draw_left_environment(jax.random.fold_in(key_list[5], 71), 0)
    right_environment = draw_right_environment(jax.random.fold_in(key_list[5], 71), 0)
    operator_blocks = scatter_about(key_list[3], (NB, S, S), 0.3, 4.0, (), jnp.float32)
    operator_pairs = place_ends(jax.random.randint(key_list[4], (NB, 2), 0, W), jax.random.fold_in(key_list[4], 1), 0, W - 1).astype(jnp.int32)
    return dict(initial_guess=initial_guess, left_environment=left_environment, right_environment=right_environment, operator_blocks=operator_blocks, operator_pairs=operator_pairs)


highest = lax.Precision.HIGHEST
epsilon = 1e-06

def lowest_pair(matrix):
    matrix_order = matrix.shape[0]
    vectors = jnp.eye(matrix_order, dtype=jnp.float32)
    for rounds in range(SWEEPS):
        for first_row in range(matrix_order):
            for second_row in range(first_row + 1, matrix_order):
                rotation_angle = 0.5 * jnp.arctan2(2.0 * matrix[first_row, second_row], matrix[second_row, second_row] - matrix[first_row, first_row])
                cosine = jnp.cos(rotation_angle)
                sine_value = jnp.sin(rotation_angle)
                rotation = jnp.eye(matrix_order, dtype=jnp.float32)
                rotation = rotation.at[first_row, first_row].set(cosine).at[second_row, second_row].set(cosine)
                rotation = rotation.at[first_row, second_row].set(sine_value).at[second_row, first_row].set(-sine_value)
                matrix = jnp.dot(rotation.T, jnp.dot(matrix, rotation, precision=highest), precision=highest)
                vectors = jnp.dot(vectors, rotation, precision=highest)
    values = jnp.diagonal(matrix)
    chosen = (jnp.arange(matrix_order, dtype=jnp.int32) == jnp.argmin(values).astype(jnp.int32)).astype(jnp.float32)
    ritz_value = jnp.sum(values * chosen)
    weights = jnp.dot(vectors, chosen, precision=highest)
    weights = jnp.where(weights[0] < 0.0, -weights, weights)
    return (ritz_value, weights)

def dense_operator(operator_blocks, operator_pairs, levels):
    symmetric = 0.5 * (operator_blocks + jnp.swapaxes(operator_blocks, 1, 2))
    indices = jnp.arange(levels, dtype=jnp.int32)
    left_hot = (operator_pairs[:, 0:1] == indices[None, :]).astype(jnp.float32)
    right_hot = (operator_pairs[:, 1:2] == indices[None, :]).astype(jnp.float32)
    return jnp.einsum('nw,nv,nts->wvts', left_hot, right_hot, symmetric, precision=highest)

def contract_right(vector_rows, right_matrix, local_operator):
    row_count, physical, window = vector_rows.shape
    levels = local_operator.shape[1]
    mixed = jnp.dot(vector_rows.reshape(row_count * physical, window), right_matrix, preferred_element_type=jnp.float32)
    mixed = mixed.reshape(row_count, physical, levels, window)
    return jnp.einsum('kvts,nsvb->kntb', local_operator, mixed, precision=highest).astype(jnp.bfloat16)

def combine(members, weights):
    total = weights[0] * members[0]
    for member_index in range(1, len(members)):
        total = total + weights[member_index] * members[member_index]
    return total

def reference(initial_guess, left_environment, right_environment, operator_blocks, operator_pairs):
    total_count = DL * S * RB
    left_matrix = left_environment.reshape(W, DL, DL)
    right_matrix = right_environment.reshape(RB, W * RB)
    operator = dense_operator(operator_blocks, operator_pairs, W)

    def apply_hamiltonian(vector):
        inner_terms = contract_right(vector.astype(jnp.bfloat16), right_matrix, operator)
        flat = inner_terms.reshape(W, DL, S * RB)
        image = jnp.zeros((DL, S * RB), jnp.float32)
        for level in range(W):
            image = image + jnp.dot(left_matrix[level], flat[level], preferred_element_type=jnp.float32)
        return image.reshape(DL, S, RB)

    def mean_product(first_array, second_array):
        return jnp.sum(first_array * second_array) / total_count
    left_diag = jnp.diagonal(left_matrix, axis1=1, axis2=2).astype(jnp.float32)
    operator_diag = jnp.diagonal(operator, axis1=2, axis2=3)
    right_diag = jnp.diagonal(right_environment, axis1=0, axis2=2).astype(jnp.float32)
    diagonal_values = jnp.einsum('ka,kvs,vb->asb', left_diag, operator_diag, right_diag, precision=highest)
    start_vector = initial_guess.astype(jnp.float32)
    basis = [start_vector * lax.rsqrt(mean_product(start_vector, start_vector) + epsilon)]
    images = [apply_hamiltonian(basis[0])]
    subspace = jnp.zeros((ITERS + 1, ITERS + 1), jnp.float32)
    subspace = subspace.at[0, 0].set(mean_product(basis[0], images[0]))
    for step_index in range(ITERS):
        filled = step_index + 1
        ritz_value, weights = lowest_pair(subspace[:filled, :filled])
        ritz_now = combine(basis, weights)
        residual_now = combine(images, weights) - ritz_value * ritz_now
        correction = residual_now / (jnp.abs(diagonal_values - ritz_value) + 1.0)
        correlations = jnp.stack([mean_product(member, correction) for member in basis])
        correction = correction - combine(basis, correlations)
        new_vector = correction * lax.rsqrt(mean_product(correction, correction) + epsilon)
        new_image = apply_hamiltonian(new_vector)
        basis.append(new_vector)
        images.append(new_image)
        row_values = jnp.stack([mean_product(member, new_image) for member in basis])
        subspace = subspace.at[filled, :filled + 1].set(row_values).at[:filled + 1, filled].set(row_values)
    ritz_value, weights = lowest_pair(subspace)
    ritz_vector = combine(basis, weights)
    residual = combine(images, weights) - ritz_value * ritz_vector
    return (ritz_vector, residual)
```

```python
import functools

import jax
import jax.numpy as jnp
from jax import lax
from jax.experimental import pallas as pl
from jax.experimental.pallas import tpu as pltpu
from jax.sharding import PartitionSpec as P

ITERS = 3
SWEEPS = 8

highest = lax.Precision.HIGHEST
epsilon = 1e-06

TILE = (8, 128)
MESH = pl.DeviceIdType.MESH


def half_angle(y, x):
    scale = jnp.maximum(jnp.abs(x), jnp.abs(y))
    zero = scale == 0.0
    inverse = 1.0 / jnp.where(zero, 1.0, scale)
    xs, ys = x * inverse, y * inverse
    h = jnp.sqrt(xs * xs + ys * ys)
    h = jnp.where(zero, 1.0, h)
    big = jnp.sqrt(0.5 * (1.0 + jnp.abs(xs) / h))
    small = 0.5 * jnp.abs(ys) / (h * big)
    positive = x >= 0.0
    cosine = jnp.where(positive, big, small)
    sine = jnp.where(positive, small, big) * jnp.where(y < 0.0, -1.0, 1.0)
    return jnp.where(zero, 1.0, cosine), jnp.where(zero, 0.0, sine)


def lowest(entries, order):
    one, none = jnp.full(TILE, 1.0, jnp.float32), jnp.full(TILE, 0.0, jnp.float32)
    if order == 1:
        return entries[(0, 0)], [one]

    def at(i, j):
        return (min(i, j), max(i, j))

    keys = [(i, j) for i in range(order) for j in range(i, order)]
    start = tuple(entries[key] for key in keys)
    vectors0 = tuple(one if i == j else none for i in range(order) for j in range(order))

    def sweep(_, carry):
        m = dict(zip(keys, carry[0]))
        v = list(carry[1])
        for p in range(order):
            for q in range(p + 1, order):
                a, b, d = m[(p, p)], m[(p, q)], m[(q, q)]
                c, s = half_angle(2.0 * b, d - a)
                m[(p, p)] = c * (c * a - s * b) - s * (c * b - s * d)
                m[(p, q)] = s * (c * a - s * b) + c * (c * b - s * d)
                m[(q, q)] = s * (s * a + c * b) + c * (s * b + c * d)
                for i in range(order):
                    if i != p and i != q:
                        x, y = m[at(i, p)], m[at(i, q)]
                        m[at(i, p)] = c * x - s * y
                        m[at(i, q)] = s * x + c * y
                    x, y = v[i * order + p], v[i * order + q]
                    v[i * order + p] = c * x - s * y
                    v[i * order + q] = s * x + c * y
        return tuple(m[key] for key in keys), tuple(v)

    values, vectors = lax.fori_loop(0, SWEEPS, sweep, (start, vectors0))
    m = dict(zip(keys, values))
    best = m[(0, 0)]
    weights = [vectors[i * order] for i in range(order)]
    for j in range(1, order):
        better = m[(j, j)] < best
        best = jnp.where(better, m[(j, j)], best)
        weights = [jnp.where(better, vectors[i * order + j], weights[i]) for i in range(order)]
    sign = jnp.where(weights[0] < 0.0, -1.0, 1.0)
    return best, [weight * sign for weight in weights]


def tiled(value, rows, columns):
    wide = jnp.concatenate([value] * (columns // 128), axis=1)
    return jnp.concatenate([wide] * (rows // 8), axis=0)


def wait_bytes(ref, sem):
    pltpu.make_async_copy(ref, ref, sem).wait()


def far_first(size):
    steps = list(range(size))
    return sorted(steps, key=lambda step: -min(step, size - step))


def davidson_kernel(sizes, guess_ref, left_hbm, joint_ref, level_ref, ritz_ref, residual_ref,
                    lv, x, y, y_own, z, part, swap_out, swap_in, rs_out, rs_in,
                    dl_mine, dl_swap, dl_all, diag, coef, sc_xy, sc_z,
                    left_sem, gather_send, gather_recv, fwd_send, fwd_recv,
                    xy_send, xy_recv, z_send, z_recv, swap_send, swap_recv,
                    rs_send, rs_recv, out_send, out_recv):
    lb, rb, wa, side, half, width, levels, total_count = sizes
    own = 2 * half
    li, ri, wi = lax.axis_index("lb"), lax.axis_index("rb"), lax.axis_index("wa")
    other = 1 - wi
    xi, yi = ri // side, ri % side
    mine = ri * 2 + wi
    order = far_first(lb)
    group = lb // 2

    def plane_peer(step):
        return ((xi + step // side) % side) * side + (yi + step % side) % side

    def plane_source(step):
        return ((xi + side - step // side) % side) * side + (yi + side - step % side) % side

    for place, step in enumerate(order):
        pltpu.make_async_copy(
            left_hbm.at[:, (li + step) % lb], lv.at[:, place], left_sem.at[place]
        ).start()

    barrier = pltpu.get_barrier_semaphore()

    def greet_plane(step, carry):
        pl.semaphore_signal(barrier, inc=1, device_id={"rb": plane_peer(step)}, device_id_type=MESH)
        return carry

    lax.fori_loop(1, rb, greet_plane, 0)

    def greet_column(step, carry):
        pl.semaphore_signal(
            barrier, inc=1,
            device_id={"lb": (li + step // 2) % lb, "wa": (wi + step) % 2},
            device_id_type=MESH,
        )
        return carry

    lax.fori_loop(1, 2 * lb, greet_column, 0)
    pl.semaphore_wait(barrier, rb - 1 + 2 * lb - 1)

    def gather_start(number, source, buf):
        def send(index, carry):
            step = rb - 1 - index
            pltpu.make_async_remote_copy(
                src_ref=source, dst_ref=buf.at[mine],
                send_sem=gather_send.at[number], recv_sem=gather_recv.at[number, step],
                device_id={"rb": plane_peer(step)}, device_id_type=MESH,
            ).start()
            return carry

        lax.fori_loop(0, rb - 1, send, 0)

    def forward(number, source, buf, slot):
        pltpu.make_async_remote_copy(
            src_ref=source, dst_ref=buf.at[slot],
            send_sem=fwd_send.at[number], recv_sem=fwd_recv.at[number],
            device_id={"wa": other}, device_id_type=MESH,
        ).start()

    def gather_forward(number, buf):
        def step_body(index, carry):
            step = rb - 1 - index
            slot = plane_source(step) * 2 + wi
            wait_bytes(buf.at[slot], gather_recv.at[number, step])
            forward(number, buf.at[slot], buf, slot)
            return carry

        lax.fori_loop(0, rb - 1, step_body, 0)

    def gather_finish(number, buf, count):
        wait_bytes(buf.at[pl.ds(0, count)], fwd_recv.at[number])
        wait_bytes(buf.at[pl.ds(0, count)], fwd_send.at[number])
        wait_bytes(buf.at[pl.ds(0, rb - 1)], gather_send.at[number])

    gather_start(0, guess_ref.at[wi], x.at[0])
    x[0, ri * 2] = guess_ref[0]
    x[0, ri * 2 + 1] = guess_ref[1]

    for place, step in enumerate(order):
        wait_bytes(lv.at[:, place], left_sem.at[place])
    per_tile = 128 // own
    lane = lax.broadcasted_iota(jnp.int32, (own, 128), 1)
    row = lax.broadcasted_iota(jnp.int32, (own, 128), 0)
    hit = lane == row + (ri % per_tile) * own
    entries = jnp.zeros((own, 128), jnp.float32)
    for level in range(levels // 2):
        block = lv[level, order.index(0), :, pl.ds(pl.multiple_of((ri // per_tile) * 128, 128), 128)]
        column = jnp.sum(jnp.where(hit, block.astype(jnp.float32), 0.0), axis=1, keepdims=True)
        entries = entries + jnp.where(lane == wi * (levels // 2) + level, column, 0.0)
    dl_mine[...] = entries.astype(jnp.bfloat16)
    swap_diag = pltpu.make_async_remote_copy(
        src_ref=dl_mine, dst_ref=dl_swap, send_sem=out_send.at[2], recv_sem=out_recv.at[2],
        device_id={"wa": other}, device_id_type=MESH,
    )
    swap_diag.start()
    gather_forward(0, x.at[0])
    swap_diag.wait()
    both = (dl_mine[...].astype(jnp.float32) + dl_swap[...].astype(jnp.float32)).astype(jnp.bfloat16)
    dl_all[ri * 2] = both[:half]
    dl_all[ri * 2 + 1] = both[half:]
    gather_start(1, dl_all.at[mine], dl_all)
    gather_finish(0, x.at[0], rb - 1)

    gram, cross, mix = {}, {}, {}
    for k in range(ITERS + 1):
        def level_body(level, carry):
            product = jnp.dot(
                lv[level].reshape(lb * own, lb_depth), x[k].reshape(lb_depth, width),
                preferred_element_type=jnp.float32,
            )
            z[:, pl.ds(pl.multiple_of(level * width, 128), width)] = product.astype(jnp.bfloat16)
            return carry

        lb_depth = rb * own
        lax.fori_loop(0, levels // 2, level_body, 0)

        def swap_copy(turn):
            rows = pl.ds(turn * group, group)
            return pltpu.make_async_remote_copy(
                src_ref=swap_out.at[rows], dst_ref=swap_in.at[rows],
                send_sem=swap_send.at[k, turn], recv_sem=swap_recv.at[k, turn],
                device_id={"wa": other}, device_id_type=MESH,
            )

        for turn in range(2):
            rows = pl.ds(turn * group * own, group * own)
            product = jnp.dot(z[rows], joint_ref[...], preferred_element_type=jnp.float32)
            part[pl.ds(turn * group, group)] = product.reshape(group, 2, half, width)
            for place in range(turn * group, (turn + 1) * group):
                swap_out[place] = part[place, other].astype(jnp.bfloat16)
            swap_copy(turn).start()

        for turn in range(2):
            swap_copy(turn).wait()
            for place in range(turn * group, (turn + 1) * group):
                step = order[place]
                if step == 0:
                    continue
                total = part[place, wi] + swap_in[place].astype(jnp.float32)
                rs_out[place] = total.astype(jnp.bfloat16)
                pltpu.make_async_remote_copy(
                    src_ref=rs_out.at[place], dst_ref=rs_in.at[place],
                    send_sem=rs_send.at[k], recv_sem=rs_recv.at[k],
                    device_id={"lb": (li + step) % lb}, device_id_type=MESH,
                ).start()
        last = order.index(0)
        image = part[last, wi] + swap_in[last].astype(jnp.float32)
        if k == 0:
            gather_forward(1, dl_all)
        wait_bytes(rs_in.at[pl.ds(0, lb - 1)], rs_recv.at[k])
        for place in range(lb - 1):
            image = image + rs_in[place].astype(jnp.float32)
        y_own[k] = image
        if k < ITERS:
            y[k, mine] = image.astype(jnp.bfloat16)

        vector = x[k, mine].astype(jnp.float32)
        rows = []

        def products(first, second):
            line = jnp.sum(first * second, axis=0, keepdims=True)
            folded = line[:, :128]
            for column in range(1, width // 128):
                folded = folded + line[:, column * 128 : (column + 1) * 128]
            return folded

        for j in range(k + 1):
            rows.append(products(x[j, mine].astype(jnp.float32), vector))
        for j in range(k + 1):
            rows.append(products(x[j, mine].astype(jnp.float32), image))
        rows += [jnp.zeros((1, 128), jnp.float32)] * (8 - len(rows))
        sc_xy[k, ri] = jnp.concatenate(rows, axis=0)

        def send_plane(index, carry):
            step = rb - 1 - index
            pltpu.make_async_remote_copy(
                src_ref=sc_xy.at[k, ri], dst_ref=sc_xy.at[k, ri],
                send_sem=xy_send.at[k], recv_sem=xy_recv.at[k],
                device_id={"rb": plane_peer(step)}, device_id_type=MESH,
            ).start()
            return carry

        lax.fori_loop(0, rb - 1, send_plane, 0)
        if k < ITERS:
            gather_start(2 + k, y.at[k, mine], y.at[k])
            forward(2 + k, y.at[k, mine], y.at[k], mine)
        wait_bytes(rs_out.at[pl.ds(0, lb - 1)], rs_send.at[k])
        wait_bytes(sc_xy.at[k, pl.ds(0, rb - 1)], xy_recv.at[k])
        summed = sc_xy[k, 0]
        for j in range(1, rb):
            summed = summed + sc_xy[k, j]
        column_mine = li * 2 + wi
        sc_z[k, column_mine] = summed

        def send_column(step, carry):
            pltpu.make_async_remote_copy(
                src_ref=sc_z.at[k, column_mine], dst_ref=sc_z.at[k, column_mine],
                send_sem=z_send.at[k], recv_sem=z_recv.at[k],
                device_id={"lb": (li + step // 2) % lb, "wa": (wi + step) % 2},
                device_id_type=MESH,
            ).start()
            return carry

        lax.fori_loop(1, 2 * lb, send_column, 0)
        if k < ITERS:
            gather_forward(2 + k, y.at[k])
        if k == 0:
            gather_finish(1, dl_all, rb - 1)
            lines = dl_all[...].reshape(2 * rb * half, 128)
            rest = level_ref[...]
            found = jnp.zeros((2 * rb * half, width), jnp.float32)
            for _ in range(3):
                term = rest.astype(jnp.bfloat16)
                rest = rest - term.astype(jnp.float32)
                found = found + jnp.dot(lines, term, preferred_element_type=jnp.float32)
            diag[...] = found.reshape(2 * rb, half, width)
        wait_bytes(sc_z.at[k, pl.ds(0, 2 * lb - 1)], z_recv.at[k])
        total = sc_z[k, 0]
        for j in range(1, 2 * lb):
            total = total + sc_z[k, j]
        total = jnp.sum(total, axis=1, keepdims=True) * (1.0 / total_count)
        scalars = [jnp.broadcast_to(total[q : q + 1], TILE) for q in range(2 * k + 2)]
        for j in range(k + 1):
            gram[(j, k)] = gram[(k, j)] = scalars[j]
            cross[(j, k)] = cross[(k, j)] = scalars[k + 1 + j]
        raw = [jnp.zeros(TILE, jnp.float32) for _ in range(k)] + [jnp.ones(TILE, jnp.float32)]
        for j in range(k):
            correlation = sum(mix[(j, i)] * gram[(i, k)] for i in range(j + 1))
            for i in range(j + 1):
                raw[i] = raw[i] - correlation * mix[(j, i)]
        norm = jnp.zeros(TILE, jnp.float32)
        for i in range(k + 1):
            norm = norm + raw[i] * sum(raw[j] * gram[(i, j)] for j in range(k + 1))
        scale = lax.rsqrt(jnp.maximum(norm, 0.0) + epsilon)
        for i in range(k + 1):
            mix[(k, i)] = raw[i] * scale
        entries = {}
        for b in range(k + 1):
            image_row = [
                sum(mix[(b, j)] * cross[(i, j)] for j in range(b + 1)) for i in range(b + 1)
            ]
            for a in range(b + 1):
                entries[(a, b)] = sum(mix[(a, i)] * image_row[i] for i in range(a + 1))
        theta, weights = lowest(entries, k + 1)
        alphas = [
            sum(weights[j] * mix[(j, i)] for j in range(i, k + 1)) for i in range(k + 1)
        ]
        for i in range(k + 1):
            coef[i] = alphas[i]
            coef[4 + i] = -(theta * alphas[i])
        coef[8] = theta

        if k < ITERS:
            gather_finish(2 + k, y.at[k], rb)

            def correct(chunk, carry):
                for start in range(0, half, 16):
                    span = pl.ds(start, 16)
                    ritz = tiled(coef[8], 16, width)
                    residual = jnp.zeros((16, width), jnp.float32)
                    for i in range(k + 1):
                        residual = residual + tiled(coef[i], 16, width) * y[i, chunk, span].astype(jnp.float32)
                        residual = residual + tiled(coef[4 + i], 16, width) * x[i, chunk, span].astype(jnp.float32)
                    below = jnp.abs(diag[chunk, span] - ritz) + 1.0
                    x[k + 1, chunk, span] = (residual / below).astype(jnp.bfloat16)
                return carry

            lax.fori_loop(0, 2 * rb, correct, 0)

    ritz_rows = jnp.zeros((half, width), jnp.float32)
    image_rows = jnp.zeros((half, width), jnp.float32)
    for i in range(ITERS + 1):
        alpha = tiled(coef[i], half, width)
        ritz_rows = ritz_rows + alpha * x[i, mine].astype(jnp.float32)
        image_rows = image_rows + alpha * y_own[i]
    ritz_ref[wi] = ritz_rows
    residual_ref[wi] = image_rows - tiled(coef[8], half, width) * ritz_rows
    copies = [
        pltpu.make_async_remote_copy(
            src_ref=ref.at[wi], dst_ref=ref.at[wi], send_sem=out_send.at[n], recv_sem=out_recv.at[n],
            device_id={"wa": other}, device_id_type=MESH,
        )
        for n, ref in enumerate((ritz_ref, residual_ref))
    ]
    for copy in copies:
        copy.start()
    wait_bytes(sc_xy.at[0, pl.ds(0, rb - 1)], xy_send.at[0])
    for k in range(1, ITERS + 1):
        wait_bytes(sc_xy.at[k, pl.ds(0, rb - 1)], xy_send.at[k])
    for k in range(ITERS + 1):
        wait_bytes(sc_z.at[k, pl.ds(0, 2 * lb - 1)], z_send.at[k])
    for copy in copies:
        copy.wait()


def dense_operator(operator_blocks, operator_pairs, levels):
    symmetric = 0.5 * (operator_blocks + jnp.swapaxes(operator_blocks, 1, 2))
    indices = jnp.arange(levels, dtype=jnp.int32)
    left_hot = (operator_pairs[:, 0:1] == indices[None, :]).astype(jnp.float32)
    right_hot = (operator_pairs[:, 1:2] == indices[None, :]).astype(jnp.float32)
    return jnp.einsum("nw,nv,nts->wvts", left_hot, right_hot, symmetric, precision=highest)


def per_device(initial_guess, left_environment, right_environment, operator_blocks, operator_pairs):
    own, physical, window = initial_guess.shape
    width = physical * window
    levels = right_environment.shape[1]
    local_levels, lb, _, _, depth = left_environment.shape
    rb, wa = lax.axis_size("rb"), lax.axis_size("wa")
    half = own // wa
    side = 1
    while side * side < rb:
        side += 1
    level_index = lax.axis_index("wa")

    operator = dense_operator(operator_blocks, operator_pairs, levels)
    local_operator = lax.dynamic_slice_in_dim(operator, level_index * local_levels, local_levels, 0)
    joint = jnp.einsum(
        "kvts,cvb->ksctb", local_operator, right_environment.astype(jnp.float32), precision=highest
    )
    joint = joint.reshape(local_levels * width, width).astype(jnp.bfloat16)
    operator_diag = jnp.diagonal(operator, axis1=2, axis2=3)
    right_diag = jnp.diagonal(right_environment, axis1=0, axis2=2).astype(jnp.float32)
    level_rows = jnp.einsum("kvs,vb->ksb", operator_diag, right_diag, precision=highest)
    level_rows = jnp.pad(level_rows.reshape(levels, width), ((0, 128 - levels), (0, 0)))

    guess = initial_guess.reshape(wa, half, width)
    left = left_environment.reshape(local_levels, lb, own, depth)
    sizes = (lb, rb, wa, side, half, width, levels, own * lb * rb * width)
    f32, bf16 = jnp.float32, jnp.bfloat16
    DMA = pltpu.SemaphoreType.DMA
    n = ITERS + 1
    vmem = pl.BlockSpec(memory_space=pltpu.VMEM)
    ritz, residual = pl.pallas_call(
        functools.partial(davidson_kernel, sizes),
        out_shape=[jax.ShapeDtypeStruct((wa, half, width), f32)] * 2,
        in_specs=[vmem, pl.BlockSpec(memory_space=pl.ANY), vmem, vmem],
        out_specs=[vmem, vmem],
        scratch_shapes=[
            pltpu.VMEM((local_levels, lb, own, depth), bf16),
            pltpu.VMEM((n, 2 * rb, half, width), bf16),
            pltpu.VMEM((ITERS, 2 * rb, half, width), bf16),
            pltpu.VMEM((n, half, width), f32),
            pltpu.VMEM((lb * own, local_levels * width), bf16),
            pltpu.VMEM((lb, 2, half, width), f32),
            pltpu.VMEM((lb, half, width), bf16),
            pltpu.VMEM((lb, half, width), bf16),
            pltpu.VMEM((lb, half, width), bf16),
            pltpu.VMEM((lb, half, width), bf16),
            pltpu.VMEM((own, 128), bf16),
            pltpu.VMEM((own, 128), bf16),
            pltpu.VMEM((2 * rb, half, 128), bf16),
            pltpu.VMEM((2 * rb, half, width), f32),
            pltpu.VMEM((9,) + TILE, f32),
            pltpu.VMEM((n, rb) + TILE, f32),
            pltpu.VMEM((n, 2 * lb) + TILE, f32),
            DMA((lb,)),
            DMA((2 + ITERS,)),
            DMA((2 + ITERS, rb)),
            DMA((2 + ITERS,)),
            DMA((2 + ITERS,)),
            DMA((n,)),
            DMA((n,)),
            DMA((n,)),
            DMA((n,)),
            DMA((n, 2)),
            DMA((n, 2)),
            DMA((n,)),
            DMA((n,)),
            DMA((3,)),
            DMA((3,)),
        ],
        compiler_params=pltpu.CompilerParams(
            collective_id=0, has_side_effects=True, vmem_limit_bytes=60 * 1024 * 1024
        ),
    )(guess, left, joint, level_rows)
    return ritz.reshape(own, physical, window), residual.reshape(own, physical, window)


def solution(mesh):
    in_specs = (P(("lb", "rb"), None, None), P("wa", None, "rb", None, "lb"), P(), P(), P())
    out_specs = (P(("lb", "rb"), None, None), P(("lb", "rb"), None, None))
    return jax.shard_map(
        per_device, mesh=mesh, in_specs=in_specs, out_specs=out_specs, check_vma=False
    )
```

```python
import functools

import jax
import jax.numpy as jnp
from jax import lax
from jax.experimental import pallas as pl
from jax.experimental.pallas import tpu as pltpu
from jax.sharding import PartitionSpec as P

ITERS = 3
SWEEPS = 8

epsilon = 1e-06

TILE = (8, 128)
MESH = pl.DeviceIdType.MESH

FAR = (4, 3, -3)
NEAR = (2, -2, 1, -1, 0)


def half_angle(y, x):
    square = x * x + y * y
    zero = square == 0.0
    inverse = lax.rsqrt(jnp.where(zero, 1.0, square))
    half = 0.5 + 0.5 * (jnp.abs(x) * inverse)
    root = lax.rsqrt(half)
    big = half * root
    small = 0.5 * (jnp.abs(y) * inverse) * root
    positive = x >= 0.0
    cosine = jnp.where(positive, big, small)
    sine = jnp.where(positive, small, big)
    sine = jnp.where(y < 0.0, -sine, sine)
    return jnp.where(zero, 1.0, cosine), jnp.where(zero, 0.0, sine)


def lowest(entries, order):
    one, none = jnp.full(TILE, 1.0, jnp.float32), jnp.full(TILE, 0.0, jnp.float32)
    if order == 1:
        return entries[(0, 0)], [one]

    def at(i, j):
        return (min(i, j), max(i, j))

    keys = [(i, j) for i in range(order) for j in range(i, order)]
    largest = functools.reduce(jnp.maximum, [jnp.abs(entries[key]) for key in keys])
    unit = jnp.where(largest == 0.0, 1.0, largest)
    start = tuple((entries[key] / unit) * 2.0**59 for key in keys)
    vectors0 = tuple(one if i == j else none for i in range(order) for j in range(order))

    def sweep(_, carry):
        m = dict(zip(keys, carry[0]))
        v = list(carry[1])
        for p in range(order):
            for q in range(p + 1, order):
                a, b, d = m[(p, p)], m[(p, q)], m[(q, q)]
                c, s = half_angle(2.0 * b, d - a)
                m[(p, p)] = c * (c * a - s * b) - s * (c * b - s * d)
                m[(p, q)] = s * (c * a - s * b) + c * (c * b - s * d)
                m[(q, q)] = s * (s * a + c * b) + c * (s * b + c * d)
                for i in range(order):
                    if i != p and i != q:
                        x, y = m[at(i, p)], m[at(i, q)]
                        m[at(i, p)] = c * x - s * y
                        m[at(i, q)] = s * x + c * y
                    x, y = v[i * order + p], v[i * order + q]
                    v[i * order + p] = c * x - s * y
                    v[i * order + q] = s * x + c * y
        return tuple(m[key] for key in keys), tuple(v)

    values, vectors = lax.fori_loop(0, SWEEPS, sweep, (start, vectors0))
    m = dict(zip(keys, values))
    best = m[(0, 0)]
    weights = [vectors[i * order] for i in range(order)]
    for j in range(1, order):
        better = m[(j, j)] < best
        best = jnp.where(better, m[(j, j)], best)
        weights = [jnp.where(better, vectors[i * order + j], weights[i]) for i in range(order)]
    sign = jnp.where(weights[0] < 0.0, -1.0, 1.0)
    return best * 2.0**-59 * unit, [weight * sign for weight in weights]


def tiled(value, rows, columns):
    wide = jnp.concatenate([value] * (columns // 128), axis=1)
    return jnp.concatenate([wide] * (rows // 8), axis=0)


def wait_bytes(ref, sem):
    pltpu.make_async_copy(ref, ref, sem).wait()


def davidson_kernel(sizes, guess_ref, left_hbm, right_ref, blocks_ref, pairs_ref, ritz_ref, residual_ref,
                    joint_ref, level_ref, right_whole, right32, right_rows, symmetric, guess_rows, lv_far, lv_near, x, y, y_own,
                    z_far, z_near, part_far, part_near, far_out, far_in, near_out, near_in,
                    relay_out, relay_in, relay4_in, rs_out, rs_in,
                    dl_mine, dl_swap, dl_all, diag, coef, sc_xy, sc_z,
                    left_sem, gather_send, gather_recv, fwd_send, fwd_recv, column_send, column_recv,
                    xy_send, xy_recv, z_send, z_recv, swap_send, swap_recv,
                    relay_send, relay_recv, relay4_recv, rs_send, rs_recv, out_send, out_recv):
    lb, rb, wa, side, half, width, window, levels, total_count = sizes
    own = 2 * half
    li, ri, wi = lax.axis_index("lb"), lax.axis_index("rb"), lax.axis_index("wa")
    other = 1 - wi
    xi, yi = lax.div(ri, side), lax.rem(ri, side)
    mine = ri * 2 + wi
    chunks = 2 * rb
    own_column = chunks + li
    xs = [lax.rem(xi + step, side) for step in range(side)]
    ys = [lax.rem(yi + step, side) for step in range(side)]
    zs = [lax.rem(li + step, lb) for step in range(lb)]
    plane_steps = sorted(
        range(1, rb),
        key=lambda step: -min(step // side, side - step // side) - min(step % side, side - step % side),
    )
    column_steps = sorted(range(1, lb), key=lambda step: -min(step, lb - step))

    def plane_peer(step):
        return xs[step // side] * side + ys[step % side]

    def plane_source(step):
        return xs[-(step // side) % side] * side + ys[-(step % side) % side]

    for steps, held, first in ((FAR, lv_far, 0), (NEAR, lv_near, len(FAR))):
        for place, step in enumerate(steps):
            pltpu.make_async_copy(
                left_hbm.at[:, (li + step + lb) % lb], held.at[:, place], left_sem.at[first + place]
            ).start()

    barrier = pltpu.get_barrier_semaphore()

    for step in plane_steps:
        pl.semaphore_signal(barrier, inc=1, device_id={"rb": plane_peer(step)}, device_id_type=MESH)
    for step in range(lb):
        for turn in range(2):
            if step or turn:
                pl.semaphore_signal(
                    barrier, inc=1,
                    device_id={"lb": zs[step], "wa": other if turn else wi}, device_id_type=MESH,
                )

    def gather_start(number, source, buf):
        for step in plane_steps:
            pltpu.make_async_remote_copy(
                src_ref=source, dst_ref=buf.at[mine],
                send_sem=gather_send.at[number], recv_sem=gather_recv.at[number, step],
                device_id={"rb": plane_peer(step)}, device_id_type=MESH,
            ).start()
        for step in column_steps:
            pltpu.make_async_remote_copy(
                src_ref=source, dst_ref=buf.at[own_column],
                send_sem=column_send.at[number], recv_sem=column_recv.at[number],
                device_id={"lb": zs[step]}, device_id_type=MESH,
            ).start()

    def forward(number, source, buf, slot):
        pltpu.make_async_remote_copy(
            src_ref=source, dst_ref=buf.at[slot],
            send_sem=fwd_send.at[number], recv_sem=fwd_recv.at[number],
            device_id={"wa": other}, device_id_type=MESH,
        ).start()

    def gather_forward(number, buf, steps):
        for step in steps:
            slot = plane_source(step) * 2 + wi
            wait_bytes(buf.at[slot], gather_recv.at[number, step])
            forward(number, buf.at[slot], buf, slot)

    def gather_finish(number, buf, count):
        wait_bytes(buf.at[pl.ds(0, count)], fwd_recv.at[number])
        wait_bytes(buf.at[pl.ds(0, lb - 1)], column_recv.at[number])

    def gather_drain(number, buf, count):
        wait_bytes(buf.at[pl.ds(0, count)], fwd_send.at[number])
        wait_bytes(buf.at[pl.ds(0, lb - 1)], column_send.at[number])
        wait_bytes(buf.at[pl.ds(0, rb - 1)], gather_send.at[number])

    own_guess = guess_ref[...].astype(jnp.float32)
    right_whole[...] = right_ref[...].astype(jnp.float32)
    for v in range(levels):
        right32[v] = right_whole[:, v, :]
    physical = width // window
    guess_rows[...] = own_guess
    for s in range(physical):
        piece = guess_rows[:, s, :].astype(jnp.bfloat16)
        for h in range(2):
            x[0, ri * 2 + h, :, s * window : (s + 1) * window] = piece[h * half : (h + 1) * half]
    x[0, own_column] = x[0, mine]

    count = blocks_ref.shape[2]
    states = [(t, s) for t in range(physical) for s in range(t, physical)]

    def symmetrize(n, carry):
        for place, (t, s) in enumerate(states):
            symmetric[n, place] = 0.5 * (blocks_ref[t, s, n] + blocks_ref[s, t, n])
        return carry

    lax.fori_loop(0, count, symmetrize, 0)
    chunk_rows = 32

    def joint_body(index, carry):
        level, chunk = index // (window // chunk_rows), index % (window // chunk_rows)
        start = pl.multiple_of(chunk * chunk_rows, chunk_rows)

        def add_block(n, sums):
            here = jnp.where(pairs_ref[0, n] == wi * (levels // 2) + level, 1.0, 0.0)
            slab = right32[pairs_ref[1, n], pl.ds(start, chunk_rows)] * here
            return tuple(total + symmetric[n, place] * slab for place, total in enumerate(sums))

        sums = lax.fori_loop(
            0, count, add_block,
            tuple(jnp.zeros((chunk_rows, window), jnp.float32) for _ in states),
        )
        for place, (t, s) in enumerate(states):
            block = sums[place].astype(jnp.bfloat16)
            for a, b in {(t, s), (s, t)}:
                joint_ref[
                    pl.ds(pl.multiple_of(level * width + a * window + start, chunk_rows), chunk_rows),
                    b * window : (b + 1) * window,
                ] = block
        return carry

    joint_steps = (levels // 2) * (window // chunk_rows)
    lax.fori_loop(0, joint_steps // 2, joint_body, 0)
    pl.semaphore_wait(barrier, rb - 1 + 2 * lb - 1)
    gather_start(0, x.at[0, mine], x.at[0])
    lax.fori_loop(joint_steps // 2, joint_steps, joint_body, 0)

    eye = lax.broadcasted_iota(jnp.int32, (window, window), 0) == lax.broadcasted_iota(
        jnp.int32, (window, window), 1
    )
    for v in range(levels):
        right_rows[v : v + 1] = jnp.sum(jnp.where(eye, right32[v], 0.0), axis=0, keepdims=True)
    level_row = lax.broadcasted_iota(jnp.int32, (levels, window), 0)

    def add_level(n, sums):
        hit = jnp.where(level_row == pairs_ref[0, n], right_rows[pl.ds(pairs_ref[1, n], 1)], 0.0)
        return tuple(total + blocks_ref[s, s, n] * hit for s, total in enumerate(sums))

    level_ref[...] = jnp.zeros_like(level_ref)
    level_ref[:levels] = jnp.concatenate(
        lax.fori_loop(0, count, add_level, tuple(jnp.zeros((levels, window), jnp.float32) for _ in range(physical))),
        axis=1,
    )

    for held, first in ((lv_far, 0), (lv_near, len(FAR))):
        for place in range(held.shape[1]):
            wait_bytes(held.at[:, place], left_sem.at[first + place])
    per_tile = 128 // own
    lane = lax.broadcasted_iota(jnp.int32, (own, 128), 1)
    row = lax.broadcasted_iota(jnp.int32, (own, 128), 0)
    hit = lane == row + (ri % per_tile) * own
    entries = jnp.zeros((own, 128), jnp.float32)
    for level in range(levels // 2):
        block = lv_near[level, NEAR.index(0), :, pl.ds(pl.multiple_of((ri // per_tile) * 128, 128), 128)]
        column = jnp.sum(jnp.where(hit, block.astype(jnp.float32), 0.0), axis=1, keepdims=True)
        entries = entries + jnp.where(lane == wi * (levels // 2) + level, column, 0.0)
    dl_mine[...] = entries.astype(jnp.bfloat16)
    swap_diag = pltpu.make_async_remote_copy(
        src_ref=dl_mine, dst_ref=dl_swap, send_sem=out_send.at[2], recv_sem=out_recv.at[2],
        device_id={"wa": other}, device_id_type=MESH,
    )
    swap_diag.start()
    gather_forward(0, x.at[0], plane_steps)
    swap_diag.wait()
    both = (dl_mine[...].astype(jnp.float32) + dl_swap[...].astype(jnp.float32)).astype(jnp.bfloat16)
    dl_all[ri * 2] = both[:half]
    dl_all[ri * 2 + 1] = both[half:]
    dl_all[own_column] = dl_all[mine]
    gather_start(1, dl_all.at[mine], dl_all)
    gather_finish(0, x.at[0], rb - 1)

    gram, cross, mix = {}, {}, {}
    for k in range(ITERS + 1):
        def left_product(held, into, first, count):
            rows = held.shape[1] * own
            product = jnp.dot(
                held[first : first + count].reshape(count * rows, lb_depth),
                x[k, :chunks].reshape(lb_depth, width),
                preferred_element_type=jnp.float32,
            ).astype(jnp.bfloat16)
            for n in range(count):
                into[:, (first + n) * width : (first + n + 1) * width] = product[n * rows : (n + 1) * rows]

        def joint_product(held, part, swap_out):
            places = part.shape[0]
            part[...] = jnp.dot(
                held[...], joint_ref[...], preferred_element_type=jnp.float32
            ).reshape(places, 2, half, width)
            for place in range(places):
                swap_out[place] = part[place, other].astype(jnp.bfloat16)

        def swap_copy(turn, swap_out, swap_in):
            return pltpu.make_async_remote_copy(
                src_ref=swap_out, dst_ref=swap_in,
                send_sem=swap_send.at[k, turn], recv_sem=swap_recv.at[k, turn],
                device_id={"wa": other}, device_id_type=MESH,
            )

        def along(source, target, send_sem, recv_sem, step):
            pltpu.make_async_remote_copy(
                src_ref=source, dst_ref=target, send_sem=send_sem, recv_sem=recv_sem,
                device_id={"lb": zs[step % lb]}, device_id_type=MESH,
            ).start()

        def products(first, second):
            return jnp.sum((first * second).reshape(half // 8, 8, width), axis=0)

        def folded(sums):
            line = jnp.sum(sums, axis=0, keepdims=True)
            short = line[:, :128]
            for column in range(1, width // 128):
                short = short + line[:, column * 128 : (column + 1) * 128]
            return short

        def add_cross(sums, total, step):
            return [
                done + products(x[j, chunks + zs[step % lb]].astype(jnp.float32), total)
                for j, done in enumerate(sums)
            ]

        lb_depth = rb * own
        held_levels = levels // 2
        left_product(lv_far, z_far, 0, held_levels)
        joint_product(z_far, part_far, far_out)
        far_swap = swap_copy(0, far_out, far_in)
        far_swap.start()
        left_product(lv_near, z_near, 0, held_levels // 2)
        far_swap.wait()
        for place in range(len(FAR)):
            total = part_far[place, wi] + far_in[place].astype(jnp.float32)
            relay_out[place] = total.astype(jnp.bfloat16)
        along(relay_out.at[0, :16], relay4_in.at[0], relay_send.at[k], relay4_recv.at[k], 2)
        along(relay_out.at[0, 16:], relay4_in.at[1], relay_send.at[k], relay4_recv.at[k], lb - 2)
        along(relay_out.at[1], relay_in.at[0], relay_send.at[k], relay_recv.at[k], 1)
        along(relay_out.at[2], relay_in.at[1], relay_send.at[k], relay_recv.at[k], lb - 1)
        cross_sums = [jnp.zeros((8, width), jnp.float32)] * (k + 1)
        for place, step in enumerate(FAR):
            total = part_far[place, wi] + far_in[place].astype(jnp.float32)
            cross_sums = add_cross(cross_sums, total, step)
        vector = x[k, mine].astype(jnp.float32)
        lines = [folded(products(x[j, mine].astype(jnp.float32), vector)) for j in range(k + 1)]
        left_product(lv_near, z_near, held_levels // 2, held_levels - held_levels // 2)
        joint_product(z_near, part_near, near_out)
        near_swap = swap_copy(1, near_out, near_in)
        near_swap.start()
        if k == 0:
            gather_forward(1, dl_all, plane_steps)
        near_swap.wait()
        for place in range(2, 4):
            total = part_near[place, wi] + near_in[place].astype(jnp.float32)
            rs_out[place] = total.astype(jnp.bfloat16)
            along(rs_out.at[place], rs_in.at[place], rs_send.at[k], rs_recv.at[k], NEAR[place])
        for place, step in enumerate(NEAR):
            total = part_near[place, wi] + near_in[place].astype(jnp.float32)
            cross_sums = add_cross(cross_sums, total, step)
        lines += [folded(sums) for sums in cross_sums]
        lines += [jnp.zeros((1, 128), jnp.float32)] * (8 - len(lines))
        sc_xy[k, ri] = jnp.concatenate(lines, axis=0)
        for step in plane_steps:
            pltpu.make_async_remote_copy(
                src_ref=sc_xy.at[k, ri], dst_ref=sc_xy.at[k, ri],
                send_sem=xy_send.at[k], recv_sem=xy_recv.at[k],
                device_id={"rb": plane_peer(step)}, device_id_type=MESH,
            ).start()
        wait_bytes(relay_in, relay_recv.at[k])
        wait_bytes(relay4_in, relay4_recv.at[k])
        for place in range(2):
            total = part_near[place, wi] + near_in[place].astype(jnp.float32)
            total = total + relay_in[place].astype(jnp.float32)
            extra = relay4_in[place].astype(jnp.float32)
            total = jnp.concatenate(
                [total[:16] + extra, total[16:]] if place == 0 else [total[:16], total[16:] + extra], axis=0
            )
            rs_out[place] = total.astype(jnp.bfloat16)
            along(rs_out.at[place], rs_in.at[place], rs_send.at[k], rs_recv.at[k], NEAR[place])

        def share_sums():
            wait_bytes(sc_xy.at[k, pl.ds(0, rb - 1)], xy_recv.at[k])
            summed = sc_xy[k, 0]
            for j in range(1, rb):
                summed = summed + sc_xy[k, j]
            sc_z[k, column_mine] = summed
            for step in range(lb):
                for turn in range(2):
                    if step or turn:
                        pltpu.make_async_remote_copy(
                            src_ref=sc_z.at[k, column_mine], dst_ref=sc_z.at[k, column_mine],
                            send_sem=z_send.at[k], recv_sem=z_recv.at[k],
                            device_id={"lb": zs[step], "wa": other if turn else wi},
                            device_id_type=MESH,
                        ).start()

        column_mine = li * 2 + wi
        if k == ITERS:
            share_sums()
        image = part_near[4, wi] + near_in[4].astype(jnp.float32)
        wait_bytes(rs_in, rs_recv.at[k])
        for place in range(4):
            image = image + rs_in[place].astype(jnp.float32)
        y_own[k] = image
        if k < ITERS:
            rounded = image.astype(jnp.bfloat16)
            y[k, mine] = rounded
            y[k, own_column] = rounded
            gather_start(2 + k, y.at[k, mine], y.at[k])
            forward(2 + k, y.at[k, mine], y.at[k], mine)
            share_sums()
        wait_bytes(rs_out, rs_send.at[k])
        wait_bytes(relay_out, relay_send.at[k])
        if k == 0:
            gather_finish(1, dl_all, rb - 1)
            rest = level_ref[...]
            found = jnp.zeros(((chunks + lb) * half, width), jnp.float32)
            for _ in range(3):
                term = rest.astype(jnp.bfloat16)
                rest = rest - term.astype(jnp.float32)
                found = found + jnp.dot(
                    dl_all[...].reshape((chunks + lb) * half, 128), term, preferred_element_type=jnp.float32
                )
            diag[...] = found.reshape(chunks + lb, half, width)
        early = len(plane_steps) // 2
        if k < ITERS:
            gather_forward(2 + k, y.at[k], plane_steps[:early])
        wait_bytes(sc_z.at[k, pl.ds(0, 2 * lb - 1)], z_recv.at[k])
        total = sc_z[k, 0]
        for j in range(1, 2 * lb):
            total = total + sc_z[k, j]
        total = jnp.sum(total, axis=1, keepdims=True) * (1.0 / total_count)
        scalars = [jnp.broadcast_to(total[q : q + 1], TILE) for q in range(2 * k + 2)]
        for j in range(k + 1):
            gram[(j, k)] = gram[(k, j)] = scalars[j]
            cross[(j, k)] = cross[(k, j)] = scalars[k + 1 + j]
        raw = [jnp.zeros(TILE, jnp.float32) for _ in range(k)] + [jnp.ones(TILE, jnp.float32)]
        for j in range(k):
            correlation = sum(mix[(j, i)] * gram[(i, k)] for i in range(j + 1))
            for i in range(j + 1):
                raw[i] = raw[i] - correlation * mix[(j, i)]
        norm = jnp.zeros(TILE, jnp.float32)
        for i in range(k + 1):
            norm = norm + raw[i] * sum(raw[j] * gram[(i, j)] for j in range(k + 1))
        scale = lax.rsqrt(jnp.maximum(norm, 0.0) + epsilon)
        for i in range(k + 1):
            mix[(k, i)] = raw[i] * scale
        entries = {}
        for b in range(k + 1):
            image_row = [
                sum(mix[(b, j)] * cross[(i, j)] for j in range(b + 1)) for i in range(b + 1)
            ]
            for a in range(b + 1):
                entries[(a, b)] = sum(mix[(a, i)] * image_row[i] for i in range(a + 1))
        theta, weights = lowest(entries, k + 1)
        alphas = [
            sum(weights[j] * mix[(j, i)] for j in range(i, k + 1)) for i in range(k + 1)
        ]
        for i in range(k + 1):
            coef[i] = alphas[i]
            coef[4 + i] = -(theta * alphas[i])
        coef[8] = theta

        if k < ITERS:
            gather_forward(2 + k, y.at[k], plane_steps[early:])
            gather_finish(2 + k, y.at[k], rb)

            def correct(chunk, carry):
                for start in range(0, half, 16):
                    span = pl.ds(start, 16)
                    ritz = tiled(coef[8], 16, width)
                    residual = jnp.zeros((16, width), jnp.float32)
                    for i in range(k + 1):
                        residual = residual + tiled(coef[i], 16, width) * y[i, chunk, span].astype(jnp.float32)
                        residual = residual + tiled(coef[4 + i], 16, width) * x[i, chunk, span].astype(jnp.float32)
                    below = jnp.abs(diag[chunk, span] - ritz) + 1.0
                    x[k + 1, chunk, span] = (residual / below).astype(jnp.bfloat16)
                return carry

            lax.fori_loop(0, chunks + lb, correct, 0)

    ritz_rows = jnp.zeros((half, width), jnp.float32)
    image_rows = jnp.zeros((half, width), jnp.float32)
    for i in range(ITERS + 1):
        alpha = tiled(coef[i], half, width)
        ritz_rows = ritz_rows + alpha * x[i, mine].astype(jnp.float32)
        image_rows = image_rows + alpha * y_own[i]
    image_rows = image_rows - tiled(coef[8], half, width) * ritz_rows
    my_rows = pl.ds(pl.multiple_of(wi * half, half), half)
    copies = []
    for n, (ref, rows) in enumerate(((ritz_ref, ritz_rows), (residual_ref, image_rows))):
        for s in range(physical):
            ref[my_rows, s, :] = rows[:, s * window : (s + 1) * window]
        copies.append(
            pltpu.make_async_remote_copy(
                src_ref=ref.at[my_rows], dst_ref=ref.at[my_rows],
                send_sem=out_send.at[n], recv_sem=out_recv.at[n],
                device_id={"wa": other}, device_id_type=MESH,
            )
        )
    for copy in copies:
        copy.start()
    gather_drain(0, x.at[0], rb - 1)
    gather_drain(1, dl_all, rb - 1)
    for k in range(ITERS):
        gather_drain(2 + k, y.at[k], rb)
    wait_bytes(sc_xy.at[0, pl.ds(0, rb - 1)], xy_send.at[0])
    for k in range(1, ITERS + 1):
        wait_bytes(sc_xy.at[k, pl.ds(0, rb - 1)], xy_send.at[k])
    for k in range(ITERS + 1):
        wait_bytes(sc_z.at[k, pl.ds(0, 2 * lb - 1)], z_send.at[k])
    for copy in copies:
        copy.wait()


def per_device(initial_guess, left_environment, right_environment, operator_blocks, operator_pairs):
    own, physical, window = initial_guess.shape
    width = physical * window
    levels = right_environment.shape[1]
    local_levels, lb, _, _, depth = left_environment.shape
    rb, wa = lax.axis_size("rb"), lax.axis_size("wa")
    half = own // wa
    side = 1
    while side * side < rb:
        side += 1
    left = left_environment.reshape(local_levels, lb, own, depth)
    sizes = (lb, rb, wa, side, half, width, window, levels, own * lb * rb * width)
    f32, bf16 = jnp.float32, jnp.bfloat16
    DMA = pltpu.SemaphoreType.DMA
    n = ITERS + 1
    vmem = pl.BlockSpec(memory_space=pltpu.VMEM)
    smem = pl.BlockSpec(memory_space=pltpu.SMEM)
    blocks = operator_blocks.shape[0]
    pairs_of_states = physical * (physical + 1) // 2
    ritz, residual = pl.pallas_call(
        functools.partial(davidson_kernel, sizes),
        out_shape=[jax.ShapeDtypeStruct((own, physical, window), f32)] * 2,
        in_specs=[vmem, pl.BlockSpec(memory_space=pl.ANY), vmem, smem, smem],
        out_specs=[vmem, vmem],
        scratch_shapes=[
            pltpu.VMEM((local_levels * width, width), bf16),
            pltpu.VMEM((128, width), f32),
            pltpu.VMEM((window, levels, window), f32),
            pltpu.VMEM((levels, window, window), f32),
            pltpu.VMEM((levels, window), f32),
            pltpu.SMEM((blocks, pairs_of_states), f32),
            pltpu.VMEM((own, physical, window), f32),
            pltpu.VMEM((local_levels, len(FAR), own, depth), bf16),
            pltpu.VMEM((local_levels, len(NEAR), own, depth), bf16),
            pltpu.VMEM((n, 2 * rb + lb, half, width), bf16),
            pltpu.VMEM((ITERS, 2 * rb + lb, half, width), bf16),
            pltpu.VMEM((n, half, width), f32),
            pltpu.VMEM((len(FAR) * own, local_levels * width), bf16),
            pltpu.VMEM((len(NEAR) * own, local_levels * width), bf16),
            pltpu.VMEM((len(FAR), 2, half, width), f32),
            pltpu.VMEM((len(NEAR), 2, half, width), f32),
            pltpu.VMEM((len(FAR), half, width), bf16),
            pltpu.VMEM((len(FAR), half, width), bf16),
            pltpu.VMEM((len(NEAR), half, width), bf16),
            pltpu.VMEM((len(NEAR), half, width), bf16),
            pltpu.VMEM((len(FAR), half, width), bf16),
            pltpu.VMEM((2, half, width), bf16),
            pltpu.VMEM((2, half // 2, width), bf16),
            pltpu.VMEM((4, half, width), bf16),
            pltpu.VMEM((4, half, width), bf16),
            pltpu.VMEM((own, 128), bf16),
            pltpu.VMEM((own, 128), bf16),
            pltpu.VMEM((2 * rb + lb, half, 128), bf16),
            pltpu.VMEM((2 * rb + lb, half, width), f32),
            pltpu.VMEM((9,) + TILE, f32),
            pltpu.VMEM((n, rb) + TILE, f32),
            pltpu.VMEM((n, 2 * lb) + TILE, f32),
            DMA((lb,)),
            DMA((2 + ITERS,)),
            DMA((2 + ITERS, rb)),
            DMA((2 + ITERS,)),
            DMA((2 + ITERS,)),
            DMA((2 + ITERS,)),
            DMA((2 + ITERS,)),
            DMA((n,)),
            DMA((n,)),
            DMA((n,)),
            DMA((n,)),
            DMA((n, 2)),
            DMA((n, 2)),
            DMA((n,)),
            DMA((n,)),
            DMA((n,)),
            DMA((n,)),
            DMA((n,)),
            DMA((3,)),
            DMA((3,)),
        ],
        compiler_params=pltpu.CompilerParams(
            collective_id=0, has_side_effects=True, vmem_limit_bytes=60 * 1024 * 1024
        ),
    )(
        initial_guess, left, right_environment,
        jnp.transpose(operator_blocks, (1, 2, 0)), jnp.transpose(operator_pairs),
    )
    return ritz, residual


def solution(mesh):
    in_specs = (P(("lb", "rb"), None, None), P("wa", None, "rb", None, "lb"), P(), P(), P())
    out_specs = (P(("lb", "rb"), None, None), P(("lb", "rb"), None, None))
    return jax.shard_map(
        per_device, mesh=mesh, in_specs=in_specs, out_specs=out_specs, check_vma=False
    )
```

```python
import functools

import jax
import jax.numpy as jnp
from jax import lax
from jax.experimental import pallas as pl
from jax.experimental.pallas import tpu as pltpu
from jax.sharding import PartitionSpec as P

ITERS = 3
SWEEPS = 8

epsilon = 1e-06

TILE = (8, 128)
MESH = pl.DeviceIdType.MESH

FAR = (4, 3, -3)
NEAR = (2, -2, 1, -1, 0)


def half_angle(y, x):
    square = x * x + y * y
    zero = square == 0.0
    inverse = lax.rsqrt(jnp.where(zero, 1.0, square))
    half = 0.5 + 0.5 * (jnp.abs(x) * inverse)
    root = lax.rsqrt(half)
    big = half * root
    small = 0.5 * (jnp.abs(y) * inverse) * root
    positive = x >= 0.0
    cosine = jnp.where(positive, big, small)
    sine = jnp.where(positive, small, big)
    sine = jnp.where(y < 0.0, -sine, sine)
    return jnp.where(zero, 1.0, cosine), jnp.where(zero, 0.0, sine)


def lowest(entries, order):
    one, none = jnp.full(TILE, 1.0, jnp.float32), jnp.full(TILE, 0.0, jnp.float32)
    if order == 1:
        return entries[(0, 0)], [one]

    def at(i, j):
        return (min(i, j), max(i, j))

    keys = [(i, j) for i in range(order) for j in range(i, order)]
    largest = functools.reduce(jnp.maximum, [jnp.abs(entries[key]) for key in keys])
    unit = jnp.where(largest == 0.0, 1.0, largest)
    start = tuple((entries[key] / unit) * 2.0**59 for key in keys)
    vectors0 = tuple(one if i == j else none for i in range(order) for j in range(order))

    def sweep(_, carry):
        m = dict(zip(keys, carry[0]))
        v = list(carry[1])
        for p in range(order):
            for q in range(p + 1, order):
                a, b, d = m[(p, p)], m[(p, q)], m[(q, q)]
                c, s = half_angle(2.0 * b, d - a)
                m[(p, p)] = c * (c * a - s * b) - s * (c * b - s * d)
                m[(p, q)] = s * (c * a - s * b) + c * (c * b - s * d)
                m[(q, q)] = s * (s * a + c * b) + c * (s * b + c * d)
                for i in range(order):
                    if i != p and i != q:
                        x, y = m[at(i, p)], m[at(i, q)]
                        m[at(i, p)] = c * x - s * y
                        m[at(i, q)] = s * x + c * y
                    x, y = v[i * order + p], v[i * order + q]
                    v[i * order + p] = c * x - s * y
                    v[i * order + q] = s * x + c * y
        return tuple(m[key] for key in keys), tuple(v)

    values, vectors = lax.fori_loop(0, SWEEPS, sweep, (start, vectors0))
    m = dict(zip(keys, values))
    best = m[(0, 0)]
    weights = [vectors[i * order] for i in range(order)]
    for j in range(1, order):
        better = m[(j, j)] < best
        best = jnp.where(better, m[(j, j)], best)
        weights = [jnp.where(better, vectors[i * order + j], weights[i]) for i in range(order)]
    sign = jnp.where(weights[0] < 0.0, -1.0, 1.0)
    return best * 2.0**-59 * unit, [weight * sign for weight in weights]


def tiled(value, rows, columns):
    wide = jnp.concatenate([value] * (columns // 128), axis=1)
    return jnp.concatenate([wide] * (rows // 8), axis=0)


def wait_bytes(ref, sem):
    pltpu.make_async_copy(ref, ref, sem).wait()


def davidson_kernel(sizes, guess_ref, left_hbm, right_ref, blocks_ref, pairs_ref, ritz_ref, residual_ref,
                    joint_ref, level_ref, right_whole, right32, right_rows, symmetric, guess_rows, lv_far, lv_near, x, y, y_own,
                    z_far, z_near, part_far, part_near, far_out, far_in, near_out, near_in,
                    relay_out, relay_in, relay4_in, rs_out, rs_in,
                    dl_mine, dl_swap, dl_all, diag, coef, sc_xy, sc_z,
                    left_sem, gather_send, gather_recv, fwd_send, fwd_recv, column_send, column_recv,
                    xy_send, xy_recv, z_send, z_recv, swap_send, swap_recv,
                    relay_send, relay_recv, relay4_recv, rs_send, rs_recv, own_send, own_recv, diag_sem):
    lb, rb, wa, side, half, width, window, levels, total_count = sizes
    own = 2 * half
    li, ri, wi = lax.axis_index("lb"), lax.axis_index("rb"), lax.axis_index("wa")
    other = 1 - wi
    xi, yi = lax.div(ri, side), lax.rem(ri, side)
    mine = ri * 2 + wi
    chunks = 2 * rb
    own_column = chunks + li
    first_at, second_at = xi + wi * (yi - xi), yi + wi * (xi - yi)
    first_unit, second_unit = side - wi * (side - 1), 1 + wi * (side - 1)
    firsts = [lax.rem(first_at + step, side) for step in range(side)]
    seconds = [lax.rem(second_at + step, side) for step in range(side)]
    zs = [lax.rem(li + step, lb) for step in range(lb)]
    ring_steps = sorted(range(1, side), key=lambda step: min(step, side - step))
    relay_steps = [(step, 0) for step in ring_steps]
    later_steps = [(a, b) for a in [0] + ring_steps for b in ring_steps]
    arrivals = relay_steps + later_steps
    column_steps = sorted(range(1, lb), key=lambda step: -min(step, lb - step))

    def plane_peer(a, b):
        return firsts[a] * first_unit + seconds[b] * second_unit

    def plane_source(a, b):
        return firsts[-a % side] * first_unit + seconds[-b % side] * second_unit

    def other_source(a, b):
        return seconds[-a % side] * second_unit + firsts[-b % side] * first_unit

    for steps, held, first in ((FAR, lv_far, 0), (NEAR, lv_near, len(FAR))):
        for place, step in enumerate(steps):
            pltpu.make_async_copy(
                left_hbm.at[:, (li + step + lb) % lb], held.at[:, place], left_sem.at[first + place]
            ).start()

    barrier = pltpu.get_barrier_semaphore()

    for a, b in arrivals:
        pl.semaphore_signal(barrier, inc=1, device_id={"rb": plane_peer(a, b)}, device_id_type=MESH)
    for step in range(lb):
        for turn in range(2):
            if step or turn:
                pl.semaphore_signal(
                    barrier, inc=1,
                    device_id={"lb": zs[step], "wa": other if turn else wi}, device_id_type=MESH,
                )

    def plane_send(number, source, buf, slot, place, a, b):
        pltpu.make_async_remote_copy(
            src_ref=source, dst_ref=buf.at[slot],
            send_sem=gather_send.at[number], recv_sem=gather_recv.at[number, place],
            device_id={"rb": plane_peer(a, b)}, device_id_type=MESH,
        ).start()

    def gather_start(number, source, buf):
        for step in ring_steps:
            plane_send(number, source, buf, mine, step * side, step, 0)
        for step in ring_steps:
            plane_send(number, source, buf, mine, step, 0, step)

    def column_start(number, source, buf):
        for step in column_steps:
            pltpu.make_async_remote_copy(
                src_ref=source, dst_ref=buf.at[own_column],
                send_sem=column_send.at[number], recv_sem=column_recv.at[number],
                device_id={"lb": zs[step]}, device_id_type=MESH,
            ).start()

    def forward(number, source, buf, slot, step):
        pltpu.make_async_remote_copy(
            src_ref=source, dst_ref=buf.at[slot],
            send_sem=fwd_send.at[number], recv_sem=fwd_recv.at[number, step],
            device_id={"wa": other}, device_id_type=MESH,
        ).start()

    def gather_relay(number, buf):
        for a, _ in relay_steps:
            slot = plane_source(a, 0) * 2 + wi
            wait_bytes(buf.at[slot], gather_recv.at[number, a * side])
            for step in ring_steps:
                plane_send(number, buf.at[slot], buf, slot, a * side + step, 0, step)
            forward(number, buf.at[slot], buf, slot, a * side)

    def gather_forward(number, buf, steps):
        for a, b in steps:
            slot = plane_source(a, b) * 2 + wi
            wait_bytes(buf.at[slot], gather_recv.at[number, a * side + b])
            forward(number, buf.at[slot], buf, slot, a * side + b)

    def gather_finish(number, buf):
        for a, b in arrivals:
            wait_bytes(buf.at[other_source(a, b) * 2 + other], fwd_recv.at[number, a * side + b])

    def pick(values, index):
        found = values[0]
        for place in range(1, len(values)):
            found = jnp.where(index == place, values[place], found)
        return found

    def column_finish(number, buf):
        wait_bytes(buf.at[pl.ds(0, lb - 1)], column_recv.at[number])

    def gather_drain(number, buf, count):
        wait_bytes(buf.at[pl.ds(0, count)], fwd_send.at[number])
        wait_bytes(buf.at[pl.ds(0, lb - 1)], column_send.at[number])
        wait_bytes(buf.at[pl.ds(0, rb - 1)], gather_send.at[number])

    own_guess = guess_ref[...].astype(jnp.float32)
    right_whole[...] = right_ref[...].astype(jnp.float32)
    for v in range(levels):
        right32[v] = right_whole[:, v, :]
    physical = width // window
    guess_rows[...] = own_guess
    for s in range(physical):
        piece = guess_rows[:, s, :].astype(jnp.bfloat16)
        for h in range(2):
            x[0, ri * 2 + h, :, s * window : (s + 1) * window] = piece[h * half : (h + 1) * half]
    x[0, own_column] = x[0, mine]

    count = blocks_ref.shape[2]
    states = [(t, s) for t in range(physical) for s in range(t, physical)]

    def symmetrize(n, carry):
        for place, (t, s) in enumerate(states):
            symmetric[n, place] = 0.5 * (blocks_ref[t, s, n] + blocks_ref[s, t, n])
        return carry

    lax.fori_loop(0, count, symmetrize, 0)
    chunk_rows = 32

    def joint_body(index, carry):
        level, chunk = index // (window // chunk_rows), index % (window // chunk_rows)
        start = pl.multiple_of(chunk * chunk_rows, chunk_rows)

        def add_block(n, sums):
            here = jnp.where(pairs_ref[0, n] == wi * (levels // 2) + level, 1.0, 0.0)
            slab = right32[pairs_ref[1, n], pl.ds(start, chunk_rows)] * here
            return tuple(total + symmetric[n, place] * slab for place, total in enumerate(sums))

        sums = lax.fori_loop(
            0, count, add_block,
            tuple(jnp.zeros((chunk_rows, window), jnp.float32) for _ in states),
        )
        for place, (t, s) in enumerate(states):
            block = sums[place].astype(jnp.bfloat16)
            for a, b in {(t, s), (s, t)}:
                joint_ref[
                    pl.ds(pl.multiple_of(level * width + a * window + start, chunk_rows), chunk_rows),
                    b * window : (b + 1) * window,
                ] = block
        return carry

    joint_steps = (levels // 2) * (window // chunk_rows)
    lax.fori_loop(0, joint_steps // 2, joint_body, 0)
    pl.semaphore_wait(barrier, rb - 1 + 2 * lb - 1)
    gather_start(0, x.at[0, mine], x.at[0])
    column_start(0, x.at[0, mine], x.at[0])
    lax.fori_loop(joint_steps // 2, joint_steps, joint_body, 0)

    eye = lax.broadcasted_iota(jnp.int32, (window, window), 0) == lax.broadcasted_iota(
        jnp.int32, (window, window), 1
    )
    for v in range(levels):
        right_rows[v : v + 1] = jnp.sum(jnp.where(eye, right32[v], 0.0), axis=0, keepdims=True)
    level_row = lax.broadcasted_iota(jnp.int32, (levels, window), 0)

    def add_level(n, sums):
        hit = jnp.where(level_row == pairs_ref[0, n], right_rows[pl.ds(pairs_ref[1, n], 1)], 0.0)
        return tuple(total + blocks_ref[s, s, n] * hit for s, total in enumerate(sums))

    level_ref[...] = jnp.zeros_like(level_ref)
    level_ref[:levels] = jnp.concatenate(
        lax.fori_loop(0, count, add_level, tuple(jnp.zeros((levels, window), jnp.float32) for _ in range(physical))),
        axis=1,
    )

    for held, first in ((lv_far, 0), (lv_near, len(FAR))):
        for place in range(held.shape[1]):
            wait_bytes(held.at[:, place], left_sem.at[first + place])
    per_tile = 128 // own
    lane = lax.broadcasted_iota(jnp.int32, (own, 128), 1)
    row = lax.broadcasted_iota(jnp.int32, (own, 128), 0)
    hit = lane == row + (ri % per_tile) * own
    entries = jnp.zeros((own, 128), jnp.float32)
    for level in range(levels // 2):
        block = lv_near[level, NEAR.index(0), :, pl.ds(pl.multiple_of((ri // per_tile) * 128, 128), 128)]
        column = jnp.sum(jnp.where(hit, block.astype(jnp.float32), 0.0), axis=1, keepdims=True)
        entries = entries + jnp.where(lane == wi * (levels // 2) + level, column, 0.0)
    dl_mine[...] = entries.astype(jnp.bfloat16)
    swap_diag = pltpu.make_async_remote_copy(
        src_ref=dl_mine, dst_ref=dl_swap, send_sem=diag_sem.at[0], recv_sem=diag_sem.at[1],
        device_id={"wa": other}, device_id_type=MESH,
    )
    swap_diag.start()
    gather_relay(0, x.at[0])
    gather_forward(0, x.at[0], later_steps)
    swap_diag.wait()
    both = (dl_mine[...].astype(jnp.float32) + dl_swap[...].astype(jnp.float32)).astype(jnp.bfloat16)
    dl_all[ri * 2] = both[:half]
    dl_all[ri * 2 + 1] = both[half:]
    dl_all[own_column] = dl_all[mine]
    gather_start(1, dl_all.at[mine], dl_all)
    column_start(1, dl_all.at[mine], dl_all)
    gather_finish(0, x.at[0])

    def correct(k, chunk, carry):
        for start in range(0, half, 16):
            span = pl.ds(start, 16)
            residual = jnp.zeros((16, width), jnp.float32)
            for i in range(k + 1):
                residual = residual + tiled(coef[i], 16, width) * y[i, chunk, span].astype(jnp.float32)
                residual = residual + tiled(coef[4 + i], 16, width) * x[i, chunk, span].astype(jnp.float32)
            below = jnp.abs(diag[chunk, span] - tiled(coef[8], 16, width)) + 1.0
            x[k + 1, chunk, span] = (residual / below).astype(jnp.bfloat16)
        return carry

    gram, cross, mix = {}, {}, {}
    for k in range(ITERS + 1):
        def left_product(held, into, first, count):
            rows = held.shape[1] * own
            product = jnp.dot(
                held[first : first + count].reshape(count * rows, lb_depth),
                x[k, :chunks].reshape(lb_depth, width),
                preferred_element_type=jnp.float32,
            ).astype(jnp.bfloat16)
            for n in range(count):
                into[:, (first + n) * width : (first + n + 1) * width] = product[n * rows : (n + 1) * rows]

        def joint_product(held, part, swap_out):
            places = part.shape[0]
            part[...] = jnp.dot(
                held[...], joint_ref[...], preferred_element_type=jnp.float32
            ).reshape(places, 2, half, width)
            for place in range(places):
                swap_out[place] = part[place, other].astype(jnp.bfloat16)

        def swap_copy(turn, swap_out, swap_in):
            return pltpu.make_async_remote_copy(
                src_ref=swap_out, dst_ref=swap_in,
                send_sem=swap_send.at[k, turn], recv_sem=swap_recv.at[k, turn],
                device_id={"wa": other}, device_id_type=MESH,
            )

        def along(source, target, send_sem, recv_sem, step):
            pltpu.make_async_remote_copy(
                src_ref=source, dst_ref=target, send_sem=send_sem, recv_sem=recv_sem,
                device_id={"lb": zs[step % lb]}, device_id_type=MESH,
            ).start()

        def products(first, second):
            return jnp.sum((first * second).reshape(half // 8, 8, width), axis=0)

        def folded(sums):
            line = jnp.sum(sums, axis=0, keepdims=True)
            short = line[:, :128]
            for column in range(1, width // 128):
                short = short + line[:, column * 128 : (column + 1) * 128]
            return short

        def add_cross(sums, total, step):
            return [
                done + products(x[j, chunks + zs[step % lb]].astype(jnp.float32), total)
                for j, done in enumerate(sums)
            ]

        lb_depth = rb * own
        held_levels = levels // 2
        left_product(lv_far, z_far, 0, held_levels)
        joint_product(z_far, part_far, far_out)
        far_swap = swap_copy(0, far_out, far_in)
        far_swap.start()
        left_product(lv_near, z_near, 0, held_levels // 2)
        if k == 0:
            column_finish(0, x.at[0])
            gather_relay(1, dl_all)
        else:
            column_finish(1 + k, y.at[k - 1])
            lax.fori_loop(chunks, chunks + lb, functools.partial(correct, k - 1), 0)
        far_swap.wait()
        for place in range(len(FAR)):
            total = part_far[place, wi] + far_in[place].astype(jnp.float32)
            relay_out[place] = total.astype(jnp.bfloat16)
        along(relay_out.at[0, :16], relay4_in.at[0], relay_send.at[k], relay4_recv.at[k], 2)
        along(relay_out.at[0, 16:], relay4_in.at[1], relay_send.at[k], relay4_recv.at[k], lb - 2)
        along(relay_out.at[1], relay_in.at[0], relay_send.at[k], relay_recv.at[k], 1)
        along(relay_out.at[2], relay_in.at[1], relay_send.at[k], relay_recv.at[k], lb - 1)
        cross_sums = [jnp.zeros((8, width), jnp.float32)] * (k + 1)
        for place, step in enumerate(FAR):
            total = part_far[place, wi] + far_in[place].astype(jnp.float32)
            cross_sums = add_cross(cross_sums, total, step)
        vector = x[k, mine].astype(jnp.float32)
        lines = [folded(products(x[j, mine].astype(jnp.float32), vector)) for j in range(k + 1)]
        left_product(lv_near, z_near, held_levels // 2, held_levels - held_levels // 2)
        joint_product(z_near, part_near, near_out)
        near_swap = swap_copy(1, near_out, near_in)
        near_swap.start()
        if k == 0:
            gather_forward(1, dl_all, later_steps)
        near_swap.wait()
        for place in range(2, 4):
            total = part_near[place, wi] + near_in[place].astype(jnp.float32)
            rs_out[place] = total.astype(jnp.bfloat16)
            along(rs_out.at[place], rs_in.at[place], rs_send.at[k], rs_recv.at[k], NEAR[place])
        for place, step in enumerate(NEAR):
            total = part_near[place, wi] + near_in[place].astype(jnp.float32)
            cross_sums = add_cross(cross_sums, total, step)
        lines += [folded(sums) for sums in cross_sums]
        lines += [jnp.zeros((1, 128), jnp.float32)] * (8 - len(lines))
        sc_xy[k, ri] = jnp.concatenate(lines, axis=0)
        for a, b in reversed(arrivals):
            pltpu.make_async_remote_copy(
                src_ref=sc_xy.at[k, ri], dst_ref=sc_xy.at[k, ri],
                send_sem=xy_send.at[k], recv_sem=xy_recv.at[k],
                device_id={"rb": plane_peer(a, b)}, device_id_type=MESH,
            ).start()
        wait_bytes(relay_in, relay_recv.at[k])
        wait_bytes(relay4_in, relay4_recv.at[k])
        for place in range(2):
            total = part_near[place, wi] + near_in[place].astype(jnp.float32)
            total = total + relay_in[place].astype(jnp.float32)
            extra = relay4_in[place].astype(jnp.float32)
            total = jnp.concatenate(
                [total[:16] + extra, total[16:]] if place == 0 else [total[:16], total[16:] + extra], axis=0
            )
            rs_out[place] = total.astype(jnp.bfloat16)
            along(rs_out.at[place], rs_in.at[place], rs_send.at[k], rs_recv.at[k], NEAR[place])

        def share_sums():
            wait_bytes(sc_xy.at[k, pl.ds(0, rb - 1)], xy_recv.at[k])
            summed = sc_xy[k, 0]
            for j in range(1, rb):
                summed = summed + sc_xy[k, j]
            sc_z[k, column_mine] = summed
            for step in range(lb):
                for turn in range(2):
                    if step or turn:
                        pltpu.make_async_remote_copy(
                            src_ref=sc_z.at[k, column_mine], dst_ref=sc_z.at[k, column_mine],
                            send_sem=z_send.at[k], recv_sem=z_recv.at[k],
                            device_id={"lb": zs[step], "wa": other if turn else wi},
                            device_id_type=MESH,
                        ).start()

        column_mine = li * 2 + wi
        if k == ITERS:
            share_sums()
        image = part_near[4, wi] + near_in[4].astype(jnp.float32)
        wait_bytes(rs_in, rs_recv.at[k])
        for place in range(4):
            image = image + rs_in[place].astype(jnp.float32)
        y_own[k, wi] = image
        pltpu.make_async_remote_copy(
            src_ref=y_own.at[k, wi], dst_ref=y_own.at[k, wi],
            send_sem=own_send.at[k], recv_sem=own_recv.at[k],
            device_id={"wa": other}, device_id_type=MESH,
        ).start()
        if k < ITERS:
            rounded = image.astype(jnp.bfloat16)
            y[k, mine] = rounded
            y[k, own_column] = rounded
            gather_start(2 + k, y.at[k, mine], y.at[k])
            forward(2 + k, y.at[k, mine], y.at[k], mine, 0)
            share_sums()
            column_start(2 + k, y.at[k, mine], y.at[k])
        wait_bytes(rs_out, rs_send.at[k])
        wait_bytes(relay_out, relay_send.at[k])
        if k < ITERS:
            gather_relay(2 + k, y.at[k])
        if k == 0:
            gather_finish(1, dl_all)
            column_finish(1, dl_all)
            rest = level_ref[...]
            found = jnp.zeros(((chunks + lb) * half, width), jnp.float32)
            for _ in range(3):
                term = rest.astype(jnp.bfloat16)
                rest = rest - term.astype(jnp.float32)
                found = found + jnp.dot(
                    dl_all[...].reshape((chunks + lb) * half, 128), term, preferred_element_type=jnp.float32
                )
            diag[...] = found.reshape(chunks + lb, half, width)
        places = [0] + [a * side + b for a, b in arrivals]
        sources = [ri] + [plane_source(a, b) for a, b in arrivals]
        other_sources = [ri] + [other_source(a, b) for a, b in arrivals]
        early = 1 + len(relay_steps) + len(ring_steps)
        if k < ITERS:
            gather_forward(2 + k, y.at[k], arrivals[len(relay_steps) : early - 1])
        wait_bytes(sc_z.at[k, pl.ds(0, 2 * lb - 1)], z_recv.at[k])
        total = sc_z[k, 0]
        for j in range(1, 2 * lb):
            total = total + sc_z[k, j]
        total = jnp.sum(total, axis=1, keepdims=True) * (1.0 / total_count)
        scalars = [jnp.broadcast_to(total[q : q + 1], TILE) for q in range(2 * k + 2)]
        for j in range(k + 1):
            gram[(j, k)] = gram[(k, j)] = scalars[j]
            cross[(j, k)] = cross[(k, j)] = scalars[k + 1 + j]
        raw = [jnp.zeros(TILE, jnp.float32) for _ in range(k)] + [jnp.ones(TILE, jnp.float32)]
        for j in range(k):
            correlation = sum(mix[(j, i)] * gram[(i, k)] for i in range(j + 1))
            for i in range(j + 1):
                raw[i] = raw[i] - correlation * mix[(j, i)]
        norm = jnp.zeros(TILE, jnp.float32)
        for i in range(k + 1):
            norm = norm + raw[i] * sum(raw[j] * gram[(i, j)] for j in range(k + 1))
        scale = lax.rsqrt(jnp.maximum(norm, 0.0) + epsilon)
        for i in range(k + 1):
            mix[(k, i)] = raw[i] * scale
        entries = {}
        for b in range(k + 1):
            image_row = [
                sum(mix[(b, j)] * cross[(i, j)] for j in range(b + 1)) for i in range(b + 1)
            ]
            for a in range(b + 1):
                entries[(a, b)] = sum(mix[(a, i)] * image_row[i] for i in range(a + 1))
        theta, weights = lowest(entries, k + 1)
        alphas = [
            sum(weights[j] * mix[(j, i)] for j in range(i, k + 1)) for i in range(k + 1)
        ]
        for i in range(k + 1):
            coef[i] = alphas[i]
            coef[4 + i] = -(theta * alphas[i])
        coef[8] = theta

        if k < ITERS:

            def correct_early(index, carry):
                return correct(k, pick(sources, index) * 2 + wi, carry)

            def correct_late(index, carry):
                slot, step = pick(sources, index) * 2 + wi, pick(places, index)
                wait_bytes(y.at[k, slot], gather_recv.at[2 + k, step])
                forward(2 + k, y.at[k, slot], y.at[k], slot, step)
                return correct(k, slot, carry)

            def correct_other(index, carry):
                slot, step = pick(other_sources, index) * 2 + other, pick(places, index)
                wait_bytes(y.at[k, slot], fwd_recv.at[2 + k, step])
                return correct(k, slot, carry)

            lax.fori_loop(0, early, correct_early, 0)
            lax.fori_loop(early, rb, correct_late, 0)
            lax.fori_loop(0, rb, correct_other, 0)

    for k in range(ITERS + 1):
        wait_bytes(y_own.at[k, other], own_recv.at[k])
    theta_rows = tiled(coef[8], half, width)
    for h in range(2):
        ritz_rows = jnp.zeros((half, width), jnp.float32)
        image_rows = jnp.zeros((half, width), jnp.float32)
        for i in range(ITERS + 1):
            alpha = tiled(coef[i], half, width)
            ritz_rows = ritz_rows + alpha * x[i, ri * 2 + h].astype(jnp.float32)
            image_rows = image_rows + alpha * y_own[i, h]
        image_rows = image_rows - theta_rows * ritz_rows
        for s in range(physical):
            ritz_ref[h * half : (h + 1) * half, s, :] = ritz_rows[:, s * window : (s + 1) * window]
            residual_ref[h * half : (h + 1) * half, s, :] = image_rows[:, s * window : (s + 1) * window]
    gather_drain(0, x.at[0], rb - 1)
    gather_drain(1, dl_all, rb - 1)
    for k in range(ITERS):
        gather_drain(2 + k, y.at[k], rb)
    wait_bytes(sc_xy.at[0, pl.ds(0, rb - 1)], xy_send.at[0])
    for k in range(1, ITERS + 1):
        wait_bytes(sc_xy.at[k, pl.ds(0, rb - 1)], xy_send.at[k])
    for k in range(ITERS + 1):
        wait_bytes(sc_z.at[k, pl.ds(0, 2 * lb - 1)], z_send.at[k])
        wait_bytes(y_own.at[k, wi], own_send.at[k])


def copy_kernel(first_in, second_in, first_out, second_out):
    first_out[...] = first_in[...]
    second_out[...] = second_in[...]


def per_device(initial_guess, left_environment, right_environment, operator_blocks, operator_pairs):
    own, physical, window = initial_guess.shape
    width = physical * window
    levels = right_environment.shape[1]
    local_levels, lb, _, _, depth = left_environment.shape
    rb, wa = lax.axis_size("rb"), lax.axis_size("wa")
    half = own // wa
    side = 1
    while side * side < rb:
        side += 1
    left = left_environment.reshape(local_levels, lb, own, depth)
    sizes = (lb, rb, wa, side, half, width, window, levels, own * lb * rb * width)
    f32, bf16 = jnp.float32, jnp.bfloat16
    DMA = pltpu.SemaphoreType.DMA
    n = ITERS + 1
    vmem = pl.BlockSpec(memory_space=pltpu.VMEM)
    smem = pl.BlockSpec(memory_space=pltpu.SMEM)
    blocks = operator_blocks.shape[0]
    pairs_of_states = physical * (physical + 1) // 2
    ritz, residual = pl.pallas_call(
        functools.partial(davidson_kernel, sizes),
        out_shape=[jax.ShapeDtypeStruct((own, physical, window), f32)] * 2,
        in_specs=[vmem, pl.BlockSpec(memory_space=pl.ANY), vmem, smem, smem],
        out_specs=[vmem, vmem],
        scratch_shapes=[
            pltpu.VMEM((local_levels * width, width), bf16),
            pltpu.VMEM((128, width), f32),
            pltpu.VMEM((window, levels, window), f32),
            pltpu.VMEM((levels, window, window), f32),
            pltpu.VMEM((levels, window), f32),
            pltpu.SMEM((blocks, pairs_of_states), f32),
            pltpu.VMEM((own, physical, window), f32),
            pltpu.VMEM((local_levels, len(FAR), own, depth), bf16),
            pltpu.VMEM((local_levels, len(NEAR), own, depth), bf16),
            pltpu.VMEM((n, 2 * rb + lb, half, width), bf16),
            pltpu.VMEM((ITERS, 2 * rb + lb, half, width), bf16),
            pltpu.VMEM((n, 2, half, width), f32),
            pltpu.VMEM((len(FAR) * own, local_levels * width), bf16),
            pltpu.VMEM((len(NEAR) * own, local_levels * width), bf16),
            pltpu.VMEM((len(FAR), 2, half, width), f32),
            pltpu.VMEM((len(NEAR), 2, half, width), f32),
            pltpu.VMEM((len(FAR), half, width), bf16),
            pltpu.VMEM((len(FAR), half, width), bf16),
            pltpu.VMEM((len(NEAR), half, width), bf16),
            pltpu.VMEM((len(NEAR), half, width), bf16),
            pltpu.VMEM((len(FAR), half, width), bf16),
            pltpu.VMEM((2, half, width), bf16),
            pltpu.VMEM((2, half // 2, width), bf16),
            pltpu.VMEM((4, half, width), bf16),
            pltpu.VMEM((4, half, width), bf16),
            pltpu.VMEM((own, 128), bf16),
            pltpu.VMEM((own, 128), bf16),
            pltpu.VMEM((2 * rb + lb, half, 128), bf16),
            pltpu.VMEM((2 * rb + lb, half, width), f32),
            pltpu.VMEM((9,) + TILE, f32),
            pltpu.VMEM((n, rb) + TILE, f32),
            pltpu.VMEM((n, 2 * lb) + TILE, f32),
            DMA((lb,)),
            DMA((2 + ITERS,)),
            DMA((2 + ITERS, rb)),
            DMA((2 + ITERS,)),
            DMA((2 + ITERS, rb)),
            DMA((2 + ITERS,)),
            DMA((2 + ITERS,)),
            DMA((n,)),
            DMA((n,)),
            DMA((n,)),
            DMA((n,)),
            DMA((n, 2)),
            DMA((n, 2)),
            DMA((n,)),
            DMA((n,)),
            DMA((n,)),
            DMA((n,)),
            DMA((n,)),
            DMA((n,)),
            DMA((n,)),
            DMA((2,)),
        ],
        compiler_params=pltpu.CompilerParams(
            collective_id=0, has_side_effects=True, vmem_limit_bytes=60 * 1024 * 1024
        ),
    )(
        initial_guess, left, right_environment,
        jnp.transpose(operator_blocks, (1, 2, 0)), jnp.transpose(operator_pairs),
    )
    return pl.pallas_call(
        copy_kernel,
        out_shape=[jax.ShapeDtypeStruct((own, physical, window), f32)] * 2,
        in_specs=[vmem, vmem],
        out_specs=[vmem, vmem],
    )(ritz, residual)


def solution(mesh):
    in_specs = (P(("lb", "rb"), None, None), P("wa", None, "rb", None, "lb"), P(), P(), P())
    out_specs = (P(("lb", "rb"), None, None), P(("lb", "rb"), None, None))
    return jax.shard_map(
        per_device, mesh=mesh, in_specs=in_specs, out_specs=out_specs, check_vma=False
    )
```

```python
import functools

import jax
import jax.numpy as jnp
from jax import lax
from jax.experimental import pallas as pl
from jax.experimental.pallas import tpu as pltpu
from jax.sharding import PartitionSpec as P

ITERS = 3
SWEEPS = 8

epsilon = 1e-06

TILE = (8, 128)
MESH = pl.DeviceIdType.MESH

FAR = (4, 3, -3)
NEAR = (2, -2, 1, -1, 0)


def half_angle(y, x):
    square = x * x + y * y
    zero = square == 0.0
    inverse = lax.rsqrt(jnp.where(zero, 1.0, square))
    half = 0.5 + 0.5 * (jnp.abs(x) * inverse)
    root = lax.rsqrt(half)
    big = half * root
    small = 0.5 * (jnp.abs(y) * inverse) * root
    positive = x >= 0.0
    cosine = jnp.where(positive, big, small)
    sine = jnp.where(positive, small, big)
    sine = jnp.where(y < 0.0, -sine, sine)
    return jnp.where(zero, 1.0, cosine), jnp.where(zero, 0.0, sine)


def lowest(entries, order):
    one, none = jnp.full(TILE, 1.0, jnp.float32), jnp.full(TILE, 0.0, jnp.float32)
    if order == 1:
        return entries[(0, 0)], [one]

    def at(i, j):
        return (min(i, j), max(i, j))

    keys = [(i, j) for i in range(order) for j in range(i, order)]
    largest = functools.reduce(jnp.maximum, [jnp.abs(entries[key]) for key in keys])
    unit = jnp.where(largest == 0.0, 1.0, largest)
    start = tuple((entries[key] / unit) * 2.0**59 for key in keys)
    vectors0 = tuple(one if i == j else none for i in range(order) for j in range(order))

    def sweep(_, carry):
        m = dict(zip(keys, carry[0]))
        v = list(carry[1])
        for p in range(order):
            for q in range(p + 1, order):
                a, b, d = m[(p, p)], m[(p, q)], m[(q, q)]
                c, s = half_angle(2.0 * b, d - a)
                m[(p, p)] = c * (c * a - s * b) - s * (c * b - s * d)
                m[(p, q)] = s * (c * a - s * b) + c * (c * b - s * d)
                m[(q, q)] = s * (s * a + c * b) + c * (s * b + c * d)
                for i in range(order):
                    if i != p and i != q:
                        x, y = m[at(i, p)], m[at(i, q)]
                        m[at(i, p)] = c * x - s * y
                        m[at(i, q)] = s * x + c * y
                    x, y = v[i * order + p], v[i * order + q]
                    v[i * order + p] = c * x - s * y
                    v[i * order + q] = s * x + c * y
        return tuple(m[key] for key in keys), tuple(v)

    values, vectors = lax.fori_loop(0, SWEEPS, sweep, (start, vectors0))
    m = dict(zip(keys, values))
    best = m[(0, 0)]
    weights = [vectors[i * order] for i in range(order)]
    for j in range(1, order):
        better = m[(j, j)] < best
        best = jnp.where(better, m[(j, j)], best)
        weights = [jnp.where(better, vectors[i * order + j], weights[i]) for i in range(order)]
    sign = jnp.where(weights[0] < 0.0, -1.0, 1.0)
    return best * 2.0**-59 * unit, [weight * sign for weight in weights]


def tiled(value, rows, columns):
    wide = jnp.concatenate([value] * (columns // 128), axis=1)
    return jnp.concatenate([wide] * (rows // 8), axis=0)


def wait_bytes(ref, sem):
    pltpu.make_async_copy(ref, ref, sem).wait()


def davidson_kernel(sizes, guess_ref, left_hbm, right_ref, blocks_ref, pairs_ref, ritz_ref, residual_ref,
                    joint_ref, level_ref, right_whole, right32, right_rows, symmetric, guess_rows, lv_far, lv_near, x, y, y_own,
                    z_far, z_near, part_far, part_near, far_out, far_in, near_out, near_in,
                    relay_out, relay_in, relay4_in, rs_out, rs_in,
                    dl_mine, dl_swap, dl_all, diag, coef, sc_xy, sc_z,
                    left_sem, gather_send, gather_recv, fwd_send, fwd_recv, column_send, column_recv,
                    xy_send, xy_recv, z_send, z_recv, swap_send, swap_recv,
                    relay_send, relay_recv, relay4_recv, rs_send, rs_recv, own_send, own_recv, diag_sem):
    lb, rb, wa, side, half, width, window, levels, total_count = sizes
    own = 2 * half
    li, ri, wi = lax.axis_index("lb"), lax.axis_index("rb"), lax.axis_index("wa")
    other = 1 - wi
    xi, yi = lax.div(ri, side), lax.rem(ri, side)
    mine = ri * 2 + wi
    chunks = 2 * rb
    own_column = chunks + li
    xs = [lax.rem(xi + step, side) for step in range(side)]
    ys = [lax.rem(yi + step, side) for step in range(side)]
    zs = [lax.rem(li + step, lb) for step in range(lb)]
    plane_steps = sorted(
        range(1, rb),
        key=lambda step: -min(step // side, side - step // side) - min(step % side, side - step % side),
    )
    column_steps = sorted(range(1, lb), key=lambda step: -min(step, lb - step))

    def plane_peer(step):
        return xs[step // side] * side + ys[step % side]

    def plane_source(step):
        return xs[-(step // side) % side] * side + ys[-(step % side) % side]

    for steps, held, first in ((FAR, lv_far, 0), (NEAR, lv_near, len(FAR))):
        for place, step in enumerate(steps):
            pltpu.make_async_copy(
                left_hbm.at[:, (li + step + lb) % lb], held.at[:, place], left_sem.at[first + place]
            ).start()

    barrier = pltpu.get_barrier_semaphore()

    for step in plane_steps:
        pl.semaphore_signal(barrier, inc=1, device_id={"rb": plane_peer(step)}, device_id_type=MESH)
    for step in range(lb):
        for turn in range(2):
            if step or turn:
                pl.semaphore_signal(
                    barrier, inc=1,
                    device_id={"lb": zs[step], "wa": other if turn else wi}, device_id_type=MESH,
                )

    def gather_start(number, source, buf):
        for step in plane_steps:
            pltpu.make_async_remote_copy(
                src_ref=source, dst_ref=buf.at[mine],
                send_sem=gather_send.at[number], recv_sem=gather_recv.at[number, step],
                device_id={"rb": plane_peer(step)}, device_id_type=MESH,
            ).start()

    def column_start(number, source, buf):
        for step in column_steps:
            pltpu.make_async_remote_copy(
                src_ref=source, dst_ref=buf.at[own_column],
                send_sem=column_send.at[number], recv_sem=column_recv.at[number],
                device_id={"lb": zs[step]}, device_id_type=MESH,
            ).start()

    def forward(number, source, buf, slot, step):
        pltpu.make_async_remote_copy(
            src_ref=source, dst_ref=buf.at[slot],
            send_sem=fwd_send.at[number], recv_sem=fwd_recv.at[number, step],
            device_id={"wa": other}, device_id_type=MESH,
        ).start()

    def gather_forward(number, buf, steps):
        for step in steps:
            slot = plane_source(step) * 2 + wi
            wait_bytes(buf.at[slot], gather_recv.at[number, step])
            forward(number, buf.at[slot], buf, slot, step)

    def gather_finish(number, buf):
        for step in plane_steps:
            wait_bytes(buf.at[plane_source(step) * 2 + other], fwd_recv.at[number, step])

    def pick(values, index):
        found = values[0]
        for place in range(1, len(values)):
            found = jnp.where(index == place, values[place], found)
        return found

    def column_finish(number, buf):
        wait_bytes(buf.at[pl.ds(0, lb - 1)], column_recv.at[number])

    def gather_drain(number, buf, count):
        wait_bytes(buf.at[pl.ds(0, count)], fwd_send.at[number])
        wait_bytes(buf.at[pl.ds(0, lb - 1)], column_send.at[number])
        wait_bytes(buf.at[pl.ds(0, rb - 1)], gather_send.at[number])

    own_guess = guess_ref[...].astype(jnp.float32)
    right_whole[...] = right_ref[...].astype(jnp.float32)
    for v in range(levels):
        right32[v] = right_whole[:, v, :]
    physical = width // window
    guess_rows[...] = own_guess
    for s in range(physical):
        piece = guess_rows[:, s, :].astype(jnp.bfloat16)
        for h in range(2):
            x[0, ri * 2 + h, :, s * window : (s + 1) * window] = piece[h * half : (h + 1) * half]
    x[0, own_column] = x[0, mine]

    count = blocks_ref.shape[2]
    states = [(t, s) for t in range(physical) for s in range(t, physical)]

    def symmetrize(n, carry):
        for place, (t, s) in enumerate(states):
            symmetric[n, place] = 0.5 * (blocks_ref[t, s, n] + blocks_ref[s, t, n])
        return carry

    lax.fori_loop(0, count, symmetrize, 0)
    chunk_rows = 32

    def joint_body(index, carry):
        level, chunk = index // (window // chunk_rows), index % (window // chunk_rows)
        start = pl.multiple_of(chunk * chunk_rows, chunk_rows)

        def add_block(n, sums):
            here = jnp.where(pairs_ref[0, n] == wi * (levels // 2) + level, 1.0, 0.0)
            slab = right32[pairs_ref[1, n], pl.ds(start, chunk_rows)] * here
            return tuple(total + symmetric[n, place] * slab for place, total in enumerate(sums))

        sums = lax.fori_loop(
            0, count, add_block,
            tuple(jnp.zeros((chunk_rows, window), jnp.float32) for _ in states),
        )
        for place, (t, s) in enumerate(states):
            block = sums[place].astype(jnp.bfloat16)
            for a, b in {(t, s), (s, t)}:
                joint_ref[
                    pl.ds(pl.multiple_of(level * width + a * window + start, chunk_rows), chunk_rows),
                    b * window : (b + 1) * window,
                ] = block
        return carry

    joint_steps = (levels // 2) * (window // chunk_rows)
    lax.fori_loop(0, joint_steps // 4, joint_body, 0)
    pl.semaphore_wait(barrier, rb - 1 + 2 * lb - 1)
    gather_start(0, x.at[0, mine], x.at[0])
    column_start(0, x.at[0, mine], x.at[0])
    lax.fori_loop(joint_steps // 4, joint_steps, joint_body, 0)

    eye = lax.broadcasted_iota(jnp.int32, (window, window), 0) == lax.broadcasted_iota(
        jnp.int32, (window, window), 1
    )
    for v in range(levels):
        right_rows[v : v + 1] = jnp.sum(jnp.where(eye, right32[v], 0.0), axis=0, keepdims=True)
    level_row = lax.broadcasted_iota(jnp.int32, (levels, window), 0)

    def add_level(n, sums):
        hit = jnp.where(level_row == pairs_ref[0, n], right_rows[pl.ds(pairs_ref[1, n], 1)], 0.0)
        return tuple(total + blocks_ref[s, s, n] * hit for s, total in enumerate(sums))

    level_ref[...] = jnp.zeros_like(level_ref)
    level_ref[:levels] = jnp.concatenate(
        lax.fori_loop(0, count, add_level, tuple(jnp.zeros((levels, window), jnp.float32) for _ in range(physical))),
        axis=1,
    )

    for held, first in ((lv_far, 0), (lv_near, len(FAR))):
        for place in range(held.shape[1]):
            wait_bytes(held.at[:, place], left_sem.at[first + place])
    per_tile = 128 // own
    lane = lax.broadcasted_iota(jnp.int32, (own, 128), 1)
    row = lax.broadcasted_iota(jnp.int32, (own, 128), 0)
    hit = lane == row + (ri % per_tile) * own
    entries = jnp.zeros((own, 128), jnp.float32)
    for level in range(levels // 2):
        block = lv_near[level, NEAR.index(0), :, pl.ds(pl.multiple_of((ri // per_tile) * 128, 128), 128)]
        column = jnp.sum(jnp.where(hit, block.astype(jnp.float32), 0.0), axis=1, keepdims=True)
        entries = entries + jnp.where(lane == wi * (levels // 2) + level, column, 0.0)
    dl_mine[...] = entries.astype(jnp.bfloat16)
    swap_diag = pltpu.make_async_remote_copy(
        src_ref=dl_mine, dst_ref=dl_swap, send_sem=diag_sem.at[0], recv_sem=diag_sem.at[1],
        device_id={"wa": other}, device_id_type=MESH,
    )
    swap_diag.start()
    gather_forward(0, x.at[0], plane_steps)
    swap_diag.wait()
    both = (dl_mine[...].astype(jnp.float32) + dl_swap[...].astype(jnp.float32)).astype(jnp.bfloat16)
    dl_all[ri * 2] = both[:half]
    dl_all[ri * 2 + 1] = both[half:]
    dl_all[own_column] = dl_all[mine]
    gather_start(1, dl_all.at[mine], dl_all)
    column_start(1, dl_all.at[mine], dl_all)
    gather_finish(0, x.at[0])

    def correct(k, chunk, carry):
        for start in range(0, half, 16):
            span = pl.ds(start, 16)
            residual = jnp.zeros((16, width), jnp.float32)
            for i in range(k + 1):
                residual = residual + tiled(coef[i], 16, width) * y[i, chunk, span].astype(jnp.float32)
                residual = residual + tiled(coef[4 + i], 16, width) * x[i, chunk, span].astype(jnp.float32)
            below = jnp.abs(diag[chunk, span] - tiled(coef[8], 16, width)) + 1.0
            x[k + 1, chunk, span] = (residual / below).astype(jnp.bfloat16)
        return carry

    gram, cross, mix = {}, {}, {}
    for k in range(ITERS + 1):
        def left_product(held, into, first, count):
            rows = held.shape[1] * own
            product = jnp.dot(
                held[first : first + count].reshape(count * rows, lb_depth),
                x[k, :chunks].reshape(lb_depth, width),
                preferred_element_type=jnp.float32,
            ).astype(jnp.bfloat16)
            for n in range(count):
                into[:, (first + n) * width : (first + n + 1) * width] = product[n * rows : (n + 1) * rows]

        def joint_product(held, part, swap_out):
            places = part.shape[0]
            part[...] = jnp.dot(
                held[...], joint_ref[...], preferred_element_type=jnp.float32
            ).reshape(places, 2, half, width)
            for place in range(places):
                swap_out[place] = part[place, other].astype(jnp.bfloat16)

        def swap_copy(turn, swap_out, swap_in):
            return pltpu.make_async_remote_copy(
                src_ref=swap_out, dst_ref=swap_in,
                send_sem=swap_send.at[k, turn], recv_sem=swap_recv.at[k, turn],
                device_id={"wa": other}, device_id_type=MESH,
            )

        def along(source, target, send_sem, recv_sem, step):
            pltpu.make_async_remote_copy(
                src_ref=source, dst_ref=target, send_sem=send_sem, recv_sem=recv_sem,
                device_id={"lb": zs[step % lb]}, device_id_type=MESH,
            ).start()

        def products(first, second):
            return jnp.sum((first * second).reshape(half // 8, 8, width), axis=0)

        def folded(sums):
            line = jnp.sum(sums, axis=0, keepdims=True)
            short = line[:, :128]
            for column in range(1, width // 128):
                short = short + line[:, column * 128 : (column + 1) * 128]
            return short

        def add_cross(sums, total, step):
            return [
                done + products(x[j, chunks + zs[step % lb]].astype(jnp.float32), total)
                for j, done in enumerate(sums)
            ]

        lb_depth = rb * own
        held_levels = levels // 2
        left_product(lv_far, z_far, 0, held_levels)
        joint_product(z_far, part_far, far_out)
        far_swap = swap_copy(0, far_out, far_in)
        far_swap.start()
        left_product(lv_near, z_near, 0, held_levels // 2)
        if k == 0:
            column_finish(0, x.at[0])
        else:
            column_finish(1 + k, y.at[k - 1])
            lax.fori_loop(chunks, chunks + lb, functools.partial(correct, k - 1), 0)
        far_swap.wait()
        for place in range(len(FAR)):
            total = part_far[place, wi] + far_in[place].astype(jnp.float32)
            relay_out[place] = total.astype(jnp.bfloat16)
        along(relay_out.at[0, :16], relay4_in.at[0], relay_send.at[k], relay4_recv.at[k], 2)
        along(relay_out.at[0, 16:], relay4_in.at[1], relay_send.at[k], relay4_recv.at[k], lb - 2)
        along(relay_out.at[1], relay_in.at[0], relay_send.at[k], relay_recv.at[k], 1)
        along(relay_out.at[2], relay_in.at[1], relay_send.at[k], relay_recv.at[k], lb - 1)
        cross_sums = [jnp.zeros((8, width), jnp.float32)] * (k + 1)
        for place, step in enumerate(FAR):
            total = part_far[place, wi] + far_in[place].astype(jnp.float32)
            cross_sums = add_cross(cross_sums, total, step)
        vector = x[k, mine].astype(jnp.float32)
        lines = [folded(products(x[j, mine].astype(jnp.float32), vector)) for j in range(k + 1)]
        left_product(lv_near, z_near, held_levels // 2, held_levels - held_levels // 2)
        joint_product(z_near, part_near, near_out)
        near_swap = swap_copy(1, near_out, near_in)
        near_swap.start()
        if k == 0:
            gather_forward(1, dl_all, plane_steps)
        near_swap.wait()
        def send_near():
            wait_bytes(relay_in, relay_recv.at[k])
            wait_bytes(relay4_in, relay4_recv.at[k])
            for place in range(4):
                total = part_near[place, wi] + near_in[place].astype(jnp.float32)
                if place < 2:
                    total = total + relay_in[place].astype(jnp.float32)
                    extra = relay4_in[place].astype(jnp.float32)
                    total = jnp.concatenate(
                        [total[:16] + extra, total[16:]] if place == 0 else [total[:16], total[16:] + extra],
                        axis=0,
                    )
                rs_out[place] = total.astype(jnp.bfloat16)
                along(rs_out.at[place], rs_in.at[place], rs_send.at[k], rs_recv.at[k], NEAR[place])

        if k < ITERS:
            send_near()
        for place, step in enumerate(NEAR):
            total = part_near[place, wi] + near_in[place].astype(jnp.float32)
            cross_sums = add_cross(cross_sums, total, step)
        lines += [folded(sums) for sums in cross_sums]
        lines += [jnp.zeros((1, 128), jnp.float32)] * (8 - len(lines))
        sc_xy[k, ri] = jnp.concatenate(lines, axis=0)
        for step in plane_steps:
            pltpu.make_async_remote_copy(
                src_ref=sc_xy.at[k, ri], dst_ref=sc_xy.at[k, ri],
                send_sem=xy_send.at[k], recv_sem=xy_recv.at[k],
                device_id={"rb": plane_peer(step)}, device_id_type=MESH,
            ).start()
        if k == ITERS:
            send_near()

        def share_sums():
            wait_bytes(sc_xy.at[k, pl.ds(0, rb - 1)], xy_recv.at[k])
            summed = sc_xy[k, 0]
            for j in range(1, rb):
                summed = summed + sc_xy[k, j]
            sc_z[k, column_mine] = summed
            for step in range(lb):
                for turn in range(2):
                    if step or turn:
                        pltpu.make_async_remote_copy(
                            src_ref=sc_z.at[k, column_mine], dst_ref=sc_z.at[k, column_mine],
                            send_sem=z_send.at[k], recv_sem=z_recv.at[k],
                            device_id={"lb": zs[step], "wa": other if turn else wi},
                            device_id_type=MESH,
                        ).start()

        column_mine = li * 2 + wi
        if k == ITERS:
            share_sums()
        image = part_near[4, wi] + near_in[4].astype(jnp.float32)
        wait_bytes(rs_in, rs_recv.at[k])
        for place in range(4):
            image = image + rs_in[place].astype(jnp.float32)
        y_own[k, wi] = image
        pltpu.make_async_remote_copy(
            src_ref=y_own.at[k, wi], dst_ref=y_own.at[k, wi],
            send_sem=own_send.at[k], recv_sem=own_recv.at[k],
            device_id={"wa": other}, device_id_type=MESH,
        ).start()
        if k < ITERS:
            rounded = image.astype(jnp.bfloat16)
            y[k, mine] = rounded
            y[k, own_column] = rounded
            gather_start(2 + k, y.at[k, mine], y.at[k])
            forward(2 + k, y.at[k, mine], y.at[k], mine, 0)
            share_sums()
            column_start(2 + k, y.at[k, mine], y.at[k])
        wait_bytes(rs_out, rs_send.at[k])
        wait_bytes(relay_out, relay_send.at[k])
        if k == 0:
            gather_finish(1, dl_all)
            column_finish(1, dl_all)
            rest = level_ref[...]
            found = jnp.zeros(((chunks + lb) * half, width), jnp.float32)
            for _ in range(3):
                term = rest.astype(jnp.bfloat16)
                rest = rest - term.astype(jnp.float32)
                found = found + jnp.dot(
                    dl_all[...].reshape((chunks + lb) * half, 128), term, preferred_element_type=jnp.float32
                )
            diag[...] = found.reshape(chunks + lb, half, width)
        arrivals = [0] + plane_steps
        sources = [ri] + [plane_source(step) for step in plane_steps]
        early = 4
        if k < ITERS:
            gather_forward(2 + k, y.at[k], arrivals[1:early])
        wait_bytes(sc_z.at[k, pl.ds(0, 2 * lb - 1)], z_recv.at[k])
        total = sc_z[k, 0]
        for j in range(1, 2 * lb):
            total = total + sc_z[k, j]
        total = jnp.sum(total, axis=1, keepdims=True) * (1.0 / total_count)
        scalars = [jnp.broadcast_to(total[q : q + 1], TILE) for q in range(2 * k + 2)]
        for j in range(k + 1):
            gram[(j, k)] = gram[(k, j)] = scalars[j]
            cross[(j, k)] = cross[(k, j)] = scalars[k + 1 + j]
        raw = [jnp.zeros(TILE, jnp.float32) for _ in range(k)] + [jnp.ones(TILE, jnp.float32)]
        for j in range(k):
            correlation = sum(mix[(j, i)] * gram[(i, k)] for i in range(j + 1))
            for i in range(j + 1):
                raw[i] = raw[i] - correlation * mix[(j, i)]
        norm = jnp.zeros(TILE, jnp.float32)
        for i in range(k + 1):
            norm = norm + raw[i] * sum(raw[j] * gram[(i, j)] for j in range(k + 1))
        scale = lax.rsqrt(jnp.maximum(norm, 0.0) + epsilon)
        for i in range(k + 1):
            mix[(k, i)] = raw[i] * scale
        entries = {}
        for b in range(k + 1):
            image_row = [
                sum(mix[(b, j)] * cross[(i, j)] for j in range(b + 1)) for i in range(b + 1)
            ]
            for a in range(b + 1):
                entries[(a, b)] = sum(mix[(a, i)] * image_row[i] for i in range(a + 1))
        theta, weights = lowest(entries, k + 1)
        alphas = [
            sum(weights[j] * mix[(j, i)] for j in range(i, k + 1)) for i in range(k + 1)
        ]
        for i in range(k + 1):
            coef[i] = alphas[i]
            coef[4 + i] = -(theta * alphas[i])
        coef[8] = theta

        if k < ITERS:

            def correct_early(index, carry):
                return correct(k, pick(sources, index) * 2 + wi, carry)

            def correct_late(index, carry):
                slot, step = pick(sources, index) * 2 + wi, pick(arrivals, index)
                wait_bytes(y.at[k, slot], gather_recv.at[2 + k, step])
                forward(2 + k, y.at[k, slot], y.at[k], slot, step)
                return correct(k, slot, carry)

            def correct_other(index, carry):
                slot, step = pick(sources, index) * 2 + other, pick(arrivals, index)
                wait_bytes(y.at[k, slot], fwd_recv.at[2 + k, step])
                return correct(k, slot, carry)

            lax.fori_loop(0, early, correct_early, 0)
            lax.fori_loop(early, rb, correct_late, 0)
            lax.fori_loop(0, rb, correct_other, 0)

    for k in range(ITERS + 1):
        wait_bytes(y_own.at[k, other], own_recv.at[k])
    theta_rows = tiled(coef[8], half, width)
    for h in range(2):
        ritz_rows = jnp.zeros((half, width), jnp.float32)
        image_rows = jnp.zeros((half, width), jnp.float32)
        for i in range(ITERS + 1):
            alpha = tiled(coef[i], half, width)
            ritz_rows = ritz_rows + alpha * x[i, ri * 2 + h].astype(jnp.float32)
            image_rows = image_rows + alpha * y_own[i, h]
        image_rows = image_rows - theta_rows * ritz_rows
        for s in range(physical):
            ritz_ref[h * half : (h + 1) * half, s, :] = ritz_rows[:, s * window : (s + 1) * window]
            residual_ref[h * half : (h + 1) * half, s, :] = image_rows[:, s * window : (s + 1) * window]
    gather_drain(0, x.at[0], rb - 1)
    gather_drain(1, dl_all, rb - 1)
    for k in range(ITERS):
        gather_drain(2 + k, y.at[k], rb)
    wait_bytes(sc_xy.at[0, pl.ds(0, rb - 1)], xy_send.at[0])
    for k in range(1, ITERS + 1):
        wait_bytes(sc_xy.at[k, pl.ds(0, rb - 1)], xy_send.at[k])
    for k in range(ITERS + 1):
        wait_bytes(sc_z.at[k, pl.ds(0, 2 * lb - 1)], z_send.at[k])
        wait_bytes(y_own.at[k, wi], own_send.at[k])


def copy_kernel(first_in, second_in, first_out, second_out):
    first_out[...] = first_in[...]
    second_out[...] = second_in[...]


def per_device(initial_guess, left_environment, right_environment, operator_blocks, operator_pairs):
    own, physical, window = initial_guess.shape
    width = physical * window
    levels = right_environment.shape[1]
    local_levels, lb, _, _, depth = left_environment.shape
    rb, wa = lax.axis_size("rb"), lax.axis_size("wa")
    half = own // wa
    side = 1
    while side * side < rb:
        side += 1
    left = left_environment.reshape(local_levels, lb, own, depth)
    sizes = (lb, rb, wa, side, half, width, window, levels, own * lb * rb * width)
    f32, bf16 = jnp.float32, jnp.bfloat16
    DMA = pltpu.SemaphoreType.DMA
    n = ITERS + 1
    vmem = pl.BlockSpec(memory_space=pltpu.VMEM)
    smem = pl.BlockSpec(memory_space=pltpu.SMEM)
    blocks = operator_blocks.shape[0]
    pairs_of_states = physical * (physical + 1) // 2
    ritz, residual = pl.pallas_call(
        functools.partial(davidson_kernel, sizes),
        out_shape=[jax.ShapeDtypeStruct((own, physical, window), f32)] * 2,
        in_specs=[vmem, pl.BlockSpec(memory_space=pl.ANY), vmem, smem, smem],
        out_specs=[vmem, vmem],
        scratch_shapes=[
            pltpu.VMEM((local_levels * width, width), bf16),
            pltpu.VMEM((128, width), f32),
            pltpu.VMEM((window, levels, window), f32),
            pltpu.VMEM((levels, window, window), f32),
            pltpu.VMEM((levels, window), f32),
            pltpu.SMEM((blocks, pairs_of_states), f32),
            pltpu.VMEM((own, physical, window), f32),
            pltpu.VMEM((local_levels, len(FAR), own, depth), bf16),
            pltpu.VMEM((local_levels, len(NEAR), own, depth), bf16),
            pltpu.VMEM((n, 2 * rb + lb, half, width), bf16),
            pltpu.VMEM((ITERS, 2 * rb + lb, half, width), bf16),
            pltpu.VMEM((n, 2, half, width), f32),
            pltpu.VMEM((len(FAR) * own, local_levels * width), bf16),
            pltpu.VMEM((len(NEAR) * own, local_levels * width), bf16),
            pltpu.VMEM((len(FAR), 2, half, width), f32),
            pltpu.VMEM((len(NEAR), 2, half, width), f32),
            pltpu.VMEM((len(FAR), half, width), bf16),
            pltpu.VMEM((len(FAR), half, width), bf16),
            pltpu.VMEM((len(NEAR), half, width), bf16),
            pltpu.VMEM((len(NEAR), half, width), bf16),
            pltpu.VMEM((len(FAR), half, width), bf16),
            pltpu.VMEM((2, half, width), bf16),
            pltpu.VMEM((2, half // 2, width), bf16),
            pltpu.VMEM((4, half, width), bf16),
            pltpu.VMEM((4, half, width), bf16),
            pltpu.VMEM((own, 128), bf16),
            pltpu.VMEM((own, 128), bf16),
            pltpu.VMEM((2 * rb + lb, half, 128), bf16),
            pltpu.VMEM((2 * rb + lb, half, width), f32),
            pltpu.VMEM((9,) + TILE, f32),
            pltpu.VMEM((n, rb) + TILE, f32),
            pltpu.VMEM((n, 2 * lb) + TILE, f32),
            DMA((lb,)),
            DMA((2 + ITERS,)),
            DMA((2 + ITERS, rb)),
            DMA((2 + ITERS,)),
            DMA((2 + ITERS, rb)),
            DMA((2 + ITERS,)),
            DMA((2 + ITERS,)),
            DMA((n,)),
            DMA((n,)),
            DMA((n,)),
            DMA((n,)),
            DMA((n, 2)),
            DMA((n, 2)),
            DMA((n,)),
            DMA((n,)),
            DMA((n,)),
            DMA((n,)),
            DMA((n,)),
            DMA((n,)),
            DMA((n,)),
            DMA((2,)),
        ],
        compiler_params=pltpu.CompilerParams(
            collective_id=0, has_side_effects=True, vmem_limit_bytes=60 * 1024 * 1024
        ),
    )(
        initial_guess, left, right_environment,
        jnp.transpose(operator_blocks, (1, 2, 0)), jnp.transpose(operator_pairs),
    )
    return pl.pallas_call(
        copy_kernel,
        out_shape=[jax.ShapeDtypeStruct((own, physical, window), f32)] * 2,
        in_specs=[vmem, vmem],
        out_specs=[vmem, vmem],
    )(ritz, residual)


def solution(mesh):
    in_specs = (P(("lb", "rb"), None, None), P("wa", None, "rb", None, "lb"), P(), P(), P())
    out_specs = (P(("lb", "rb"), None, None), P(("lb", "rb"), None, None))
    return jax.shard_map(
        per_device, mesh=mesh, in_specs=in_specs, out_specs=out_specs, check_vma=False
    )
```

```python
import functools

import jax
import jax.numpy as jnp
from jax import lax
from jax.experimental import pallas as pl
from jax.experimental.pallas import tpu as pltpu
from jax.sharding import PartitionSpec as P

ITERS = 3
SWEEPS = 8

epsilon = 1e-06

TILE = (8, 128)
MESH = pl.DeviceIdType.MESH

FAR = (4, 3, -3)
NEAR = (2, -2, 1, -1, 0)


def half_angle(y, x):
    square = x * x + y * y
    zero = square == 0.0
    inverse = lax.rsqrt(jnp.where(zero, 1.0, square))
    half = 0.5 + 0.5 * (jnp.abs(x) * inverse)
    root = lax.rsqrt(half)
    big = half * root
    small = 0.5 * (jnp.abs(y) * inverse) * root
    positive = x >= 0.0
    cosine = jnp.where(positive, big, small)
    sine = jnp.where(positive, small, big)
    sine = jnp.where(y < 0.0, -sine, sine)
    return jnp.where(zero, 1.0, cosine), jnp.where(zero, 0.0, sine)


def lowest(entries, order):
    one, none = jnp.full(TILE, 1.0, jnp.float32), jnp.full(TILE, 0.0, jnp.float32)
    if order == 1:
        return entries[(0, 0)], [one]

    def at(i, j):
        return (min(i, j), max(i, j))

    keys = [(i, j) for i in range(order) for j in range(i, order)]
    largest = functools.reduce(jnp.maximum, [jnp.abs(entries[key]) for key in keys])
    unit = jnp.where(largest == 0.0, 1.0, largest)
    start = tuple((entries[key] / unit) * 2.0**59 for key in keys)
    vectors0 = tuple(one if i == j else none for i in range(order) for j in range(order))

    def sweep(_, carry):
        m = dict(zip(keys, carry[0]))
        v = list(carry[1])
        for p in range(order):
            for q in range(p + 1, order):
                a, b, d = m[(p, p)], m[(p, q)], m[(q, q)]
                c, s = half_angle(2.0 * b, d - a)
                m[(p, p)] = c * (c * a - s * b) - s * (c * b - s * d)
                m[(p, q)] = s * (c * a - s * b) + c * (c * b - s * d)
                m[(q, q)] = s * (s * a + c * b) + c * (s * b + c * d)
                for i in range(order):
                    if i != p and i != q:
                        x, y = m[at(i, p)], m[at(i, q)]
                        m[at(i, p)] = c * x - s * y
                        m[at(i, q)] = s * x + c * y
                    x, y = v[i * order + p], v[i * order + q]
                    v[i * order + p] = c * x - s * y
                    v[i * order + q] = s * x + c * y
        return tuple(m[key] for key in keys), tuple(v)

    values, vectors = lax.fori_loop(0, SWEEPS, sweep, (start, vectors0))
    m = dict(zip(keys, values))
    best = m[(0, 0)]
    weights = [vectors[i * order] for i in range(order)]
    for j in range(1, order):
        better = m[(j, j)] < best
        best = jnp.where(better, m[(j, j)], best)
        weights = [jnp.where(better, vectors[i * order + j], weights[i]) for i in range(order)]
    sign = jnp.where(weights[0] < 0.0, -1.0, 1.0)
    return best * 2.0**-59 * unit, [weight * sign for weight in weights]


def tiled(value, rows, columns):
    wide = jnp.concatenate([value] * (columns // 128), axis=1)
    return jnp.concatenate([wide] * (rows // 8), axis=0)


def wait_bytes(ref, sem):
    pltpu.make_async_copy(ref, ref, sem).wait()


def davidson_kernel(sizes, guess_ref, left_hbm, right_ref, blocks_ref, pairs_ref, ritz_ref, residual_ref,
                    joint_ref, level_ref, right_whole, right32, right_rows, symmetric, guess_rows, lv_far, lv_near, x, y, y_own,
                    z_far, z_near, part_far, part_near, far_out, far_in, near_out, near_in,
                    relay_out, relay_in, relay4_in, rs_out, rs_in,
                    dl_mine, dl_swap, dl_all, diag, coef, sc_xy, sc_z,
                    left_sem, gather_send, gather_recv, fwd_send, fwd_recv, column_send, column_recv,
                    xy_send, xy_recv, z_send, z_recv, swap_send, swap_recv,
                    relay_send, relay_recv, relay4_recv, rs_send, rs_recv, own_send, own_recv, diag_sem):
    lb, rb, wa, side, half, width, window, levels, total_count = sizes
    own = 2 * half
    li, ri, wi = lax.axis_index("lb"), lax.axis_index("rb"), lax.axis_index("wa")
    other = 1 - wi
    xi, yi = lax.div(ri, side), lax.rem(ri, side)
    mine = ri * 2 + wi
    chunks = 2 * rb
    own_column = chunks + li
    xs = [lax.rem(xi + step, side) for step in range(side)]
    ys = [lax.rem(yi + step, side) for step in range(side)]
    zs = [lax.rem(li + step, lb) for step in range(lb)]
    plane_steps = sorted(
        range(1, rb),
        key=lambda step: -min(step // side, side - step // side) - min(step % side, side - step % side),
    )
    column_steps = sorted(range(1, lb), key=lambda step: -min(step, lb - step))

    def plane_peer(step):
        return xs[step // side] * side + ys[step % side]

    def plane_source(step):
        return xs[-(step // side) % side] * side + ys[-(step % side) % side]

    for steps, held, first in ((FAR, lv_far, 0), (NEAR, lv_near, len(FAR))):
        for place, step in enumerate(steps):
            pltpu.make_async_copy(
                left_hbm.at[:, (li + step + lb) % lb], held.at[:, place], left_sem.at[first + place]
            ).start()

    barrier = pltpu.get_barrier_semaphore()

    for step in plane_steps:
        pl.semaphore_signal(barrier, inc=1, device_id={"rb": plane_peer(step)}, device_id_type=MESH)
    for step in range(lb):
        for turn in range(2):
            if step or turn:
                pl.semaphore_signal(
                    barrier, inc=1,
                    device_id={"lb": zs[step], "wa": other if turn else wi}, device_id_type=MESH,
                )

    def gather_start(number, source, buf):
        for step in plane_steps:
            pltpu.make_async_remote_copy(
                src_ref=source, dst_ref=buf.at[mine],
                send_sem=gather_send.at[number], recv_sem=gather_recv.at[number, step],
                device_id={"rb": plane_peer(step)}, device_id_type=MESH,
            ).start()

    def column_start(number, source, buf):
        for step in column_steps:
            pltpu.make_async_remote_copy(
                src_ref=source, dst_ref=buf.at[own_column],
                send_sem=column_send.at[number], recv_sem=column_recv.at[number],
                device_id={"lb": zs[step]}, device_id_type=MESH,
            ).start()

    def forward(number, source, buf, slot, step):
        pltpu.make_async_remote_copy(
            src_ref=source, dst_ref=buf.at[slot],
            send_sem=fwd_send.at[number], recv_sem=fwd_recv.at[number, step],
            device_id={"wa": other}, device_id_type=MESH,
        ).start()

    def gather_forward(number, buf, steps):
        for step in steps:
            slot = plane_source(step) * 2 + wi
            wait_bytes(buf.at[slot], gather_recv.at[number, step])
            forward(number, buf.at[slot], buf, slot, step)

    def gather_finish(number, buf):
        for step in plane_steps:
            wait_bytes(buf.at[plane_source(step) * 2 + other], fwd_recv.at[number, step])

    def source_of(step):
        a, b = lax.div(step, side), lax.rem(step, side)
        return lax.rem(xi + side - a, side) * side + lax.rem(yi + side - b, side)

    def pick(values, index):
        found = values[0]
        for place in range(1, len(values)):
            found = jnp.where(index == place, values[place], found)
        return found

    def column_finish(number, buf):
        wait_bytes(buf.at[pl.ds(0, lb - 1)], column_recv.at[number])

    def gather_drain(number, buf, count):
        wait_bytes(buf.at[pl.ds(0, count)], fwd_send.at[number])
        wait_bytes(buf.at[pl.ds(0, lb - 1)], column_send.at[number])
        wait_bytes(buf.at[pl.ds(0, rb - 1)], gather_send.at[number])

    own_guess = guess_ref[...].astype(jnp.float32)
    right_whole[...] = right_ref[...].astype(jnp.float32)
    for v in range(levels):
        right32[v] = right_whole[:, v, :]
    physical = width // window
    guess_rows[...] = own_guess
    for s in range(physical):
        piece = guess_rows[:, s, :].astype(jnp.bfloat16)
        for h in range(2):
            x[0, ri * 2 + h, :, s * window : (s + 1) * window] = piece[h * half : (h + 1) * half]
    x[0, own_column] = x[0, mine]

    count = blocks_ref.shape[2]
    states = [(t, s) for t in range(physical) for s in range(t, physical)]

    def symmetrize(n, carry):
        for place, (t, s) in enumerate(states):
            symmetric[n, place] = 0.5 * (blocks_ref[t, s, n] + blocks_ref[s, t, n])
        return carry

    lax.fori_loop(0, count, symmetrize, 0)
    chunk_rows = 32

    def joint_body(index, carry):
        level, chunk = index // (window // chunk_rows), index % (window // chunk_rows)
        start = pl.multiple_of(chunk * chunk_rows, chunk_rows)

        def add_block(n, sums):
            here = jnp.where(pairs_ref[0, n] == wi * (levels // 2) + level, 1.0, 0.0)
            slab = right32[pairs_ref[1, n], pl.ds(start, chunk_rows)] * here
            return tuple(total + symmetric[n, place] * slab for place, total in enumerate(sums))

        sums = lax.fori_loop(
            0, count, add_block,
            tuple(jnp.zeros((chunk_rows, window), jnp.float32) for _ in states),
        )
        for place, (t, s) in enumerate(states):
            block = sums[place].astype(jnp.bfloat16)
            for a, b in {(t, s), (s, t)}:
                joint_ref[
                    pl.ds(pl.multiple_of(level * width + a * window + start, chunk_rows), chunk_rows),
                    b * window : (b + 1) * window,
                ] = block
        return carry

    joint_steps = (levels // 2) * (window // chunk_rows)
    lax.fori_loop(0, joint_steps // 4, joint_body, 0)
    pl.semaphore_wait(barrier, rb - 1 + 2 * lb - 1)
    gather_start(0, x.at[0, mine], x.at[0])
    column_start(0, x.at[0, mine], x.at[0])
    lax.fori_loop(joint_steps // 4, joint_steps, joint_body, 0)

    eye = lax.broadcasted_iota(jnp.int32, (window, window), 0) == lax.broadcasted_iota(
        jnp.int32, (window, window), 1
    )
    for v in range(levels):
        right_rows[v : v + 1] = jnp.sum(jnp.where(eye, right32[v], 0.0), axis=0, keepdims=True)
    level_row = lax.broadcasted_iota(jnp.int32, (levels, window), 0)

    def add_level(n, sums):
        hit = jnp.where(level_row == pairs_ref[0, n], right_rows[pl.ds(pairs_ref[1, n], 1)], 0.0)
        return tuple(total + blocks_ref[s, s, n] * hit for s, total in enumerate(sums))

    level_ref[...] = jnp.zeros_like(level_ref)
    level_ref[:levels] = jnp.concatenate(
        lax.fori_loop(0, count, add_level, tuple(jnp.zeros((levels, window), jnp.float32) for _ in range(physical))),
        axis=1,
    )

    for held, first in ((lv_far, 0), (lv_near, len(FAR))):
        for place in range(held.shape[1]):
            wait_bytes(held.at[:, place], left_sem.at[first + place])
    per_tile = 128 // own
    lane = lax.broadcasted_iota(jnp.int32, (own, 128), 1)
    row = lax.broadcasted_iota(jnp.int32, (own, 128), 0)
    hit = lane == row + (ri % per_tile) * own
    entries = jnp.zeros((own, 128), jnp.float32)
    for level in range(levels // 2):
        block = lv_near[level, NEAR.index(0), :, pl.ds(pl.multiple_of((ri // per_tile) * 128, 128), 128)]
        column = jnp.sum(jnp.where(hit, block.astype(jnp.float32), 0.0), axis=1, keepdims=True)
        entries = entries + jnp.where(lane == wi * (levels // 2) + level, column, 0.0)
    dl_mine[...] = entries.astype(jnp.bfloat16)
    swap_diag = pltpu.make_async_remote_copy(
        src_ref=dl_mine, dst_ref=dl_swap, send_sem=diag_sem.at[0], recv_sem=diag_sem.at[1],
        device_id={"wa": other}, device_id_type=MESH,
    )
    swap_diag.start()
    gather_forward(0, x.at[0], plane_steps)
    swap_diag.wait()
    both = (dl_mine[...].astype(jnp.float32) + dl_swap[...].astype(jnp.float32)).astype(jnp.bfloat16)
    dl_all[ri * 2] = both[:half]
    dl_all[ri * 2 + 1] = both[half:]
    dl_all[own_column] = dl_all[mine]
    gather_start(1, dl_all.at[mine], dl_all)
    column_start(1, dl_all.at[mine], dl_all)
    gather_finish(0, x.at[0])

    def correct(k, chunk, carry):
        for start in range(0, half, 16):
            span = pl.ds(start, 16)
            residual = jnp.zeros((16, width), jnp.float32)
            for i in range(k + 1):
                residual = residual + tiled(coef[i], 16, width) * y[i, chunk, span].astype(jnp.float32)
                residual = residual + tiled(coef[4 + i], 16, width) * x[i, chunk, span].astype(jnp.float32)
            below = jnp.abs(diag[chunk, span] - tiled(coef[8], 16, width)) + 1.0
            x[k + 1, chunk, span] = (residual / below).astype(jnp.bfloat16)
        return carry

    gram, cross, mix = {}, {}, {}
    for k in range(ITERS + 1):
        def left_product(held, into, first, count):
            rows = held.shape[1] * own
            product = jnp.dot(
                held[first : first + count].reshape(count * rows, lb_depth),
                x[k, :chunks].reshape(lb_depth, width),
                preferred_element_type=jnp.float32,
            ).astype(jnp.bfloat16)
            for n in range(count):
                into[:, (first + n) * width : (first + n + 1) * width] = product[n * rows : (n + 1) * rows]

        def joint_product(held, part, swap_out):
            places = part.shape[0]
            part[...] = jnp.dot(
                held[...], joint_ref[...], preferred_element_type=jnp.float32
            ).reshape(places, 2, half, width)
            for place in range(places):
                swap_out[place] = part[place, other].astype(jnp.bfloat16)

        def swap_copy(turn, swap_out, swap_in):
            return pltpu.make_async_remote_copy(
                src_ref=swap_out, dst_ref=swap_in,
                send_sem=swap_send.at[k, turn], recv_sem=swap_recv.at[k, turn],
                device_id={"wa": other}, device_id_type=MESH,
            )

        def along(source, target, send_sem, recv_sem, step):
            pltpu.make_async_remote_copy(
                src_ref=source, dst_ref=target, send_sem=send_sem, recv_sem=recv_sem,
                device_id={"lb": zs[step % lb]}, device_id_type=MESH,
            ).start()

        def products(first, second):
            return jnp.sum((first * second).reshape(half // 8, 8, width), axis=0)

        def folded(sums):
            line = jnp.sum(sums, axis=0, keepdims=True)
            short = line[:, :128]
            for column in range(1, width // 128):
                short = short + line[:, column * 128 : (column + 1) * 128]
            return short

        def add_cross(sums, total, step):
            return [
                done + products(x[j, chunks + zs[step % lb]].astype(jnp.float32), total)
                for j, done in enumerate(sums)
            ]

        lb_depth = rb * own
        held_levels = levels // 2
        left_product(lv_far, z_far, 0, held_levels)
        joint_product(z_far, part_far, far_out)
        far_swap = swap_copy(0, far_out, far_in)
        far_swap.start()
        left_product(lv_near, z_near, 0, held_levels // 2)
        if k == 0:
            column_finish(0, x.at[0])
        else:
            column_finish(1 + k, y.at[k - 1])
            lax.fori_loop(chunks, chunks + lb, functools.partial(correct, k - 1), 0)
        far_swap.wait()
        for place in range(len(FAR)):
            total = part_far[place, wi] + far_in[place].astype(jnp.float32)
            relay_out[place] = total.astype(jnp.bfloat16)
        along(relay_out.at[0, :16], relay4_in.at[0], relay_send.at[k], relay4_recv.at[k], 2)
        along(relay_out.at[0, 16:], relay4_in.at[1], relay_send.at[k], relay4_recv.at[k], lb - 2)
        along(relay_out.at[1], relay_in.at[0], relay_send.at[k], relay_recv.at[k], 1)
        along(relay_out.at[2], relay_in.at[1], relay_send.at[k], relay_recv.at[k], lb - 1)
        cross_sums = [jnp.zeros((8, width), jnp.float32)] * (k + 1)
        for place, step in enumerate(FAR):
            total = part_far[place, wi] + far_in[place].astype(jnp.float32)
            cross_sums = add_cross(cross_sums, total, step)
        vector = x[k, mine].astype(jnp.float32)
        lines = [folded(products(x[j, mine].astype(jnp.float32), vector)) for j in range(k + 1)]
        left_product(lv_near, z_near, held_levels // 2, held_levels - held_levels // 2)
        joint_product(z_near, part_near, near_out)
        near_swap = swap_copy(1, near_out, near_in)
        near_swap.start()
        if k == 0:
            gather_forward(1, dl_all, plane_steps)
        near_swap.wait()
        def send_near():
            wait_bytes(relay_in, relay_recv.at[k])
            wait_bytes(relay4_in, relay4_recv.at[k])
            for place in range(4):
                total = part_near[place, wi] + near_in[place].astype(jnp.float32)
                if place < 2:
                    total = total + relay_in[place].astype(jnp.float32)
                    extra = relay4_in[place].astype(jnp.float32)
                    total = jnp.concatenate(
                        [total[:16] + extra, total[16:]] if place == 0 else [total[:16], total[16:] + extra],
                        axis=0,
                    )
                rs_out[place] = total.astype(jnp.bfloat16)
                along(rs_out.at[place], rs_in.at[place], rs_send.at[k], rs_recv.at[k], NEAR[place])

        if k < ITERS:
            send_near()
        for place, step in enumerate(NEAR):
            total = part_near[place, wi] + near_in[place].astype(jnp.float32)
            cross_sums = add_cross(cross_sums, total, step)
        lines += [folded(sums) for sums in cross_sums]
        lines += [jnp.zeros((1, 128), jnp.float32)] * (8 - len(lines))
        sc_xy[k, ri] = jnp.concatenate(lines, axis=0)
        for step in plane_steps:
            pltpu.make_async_remote_copy(
                src_ref=sc_xy.at[k, ri], dst_ref=sc_xy.at[k, ri],
                send_sem=xy_send.at[k], recv_sem=xy_recv.at[k],
                device_id={"rb": plane_peer(step)}, device_id_type=MESH,
            ).start()
        if k == ITERS:
            send_near()

        def share_sums():
            wait_bytes(sc_xy.at[k, pl.ds(0, rb - 1)], xy_recv.at[k])
            summed = sc_xy[k, 0]
            for j in range(1, rb):
                summed = summed + sc_xy[k, j]
            sc_z[k, column_mine] = summed
            for step in range(lb):
                for turn in range(2):
                    if step or turn:
                        pltpu.make_async_remote_copy(
                            src_ref=sc_z.at[k, column_mine], dst_ref=sc_z.at[k, column_mine],
                            send_sem=z_send.at[k], recv_sem=z_recv.at[k],
                            device_id={"lb": zs[step], "wa": other if turn else wi},
                            device_id_type=MESH,
                        ).start()

        column_mine = li * 2 + wi
        if k == ITERS:
            share_sums()
        image = part_near[4, wi] + near_in[4].astype(jnp.float32)
        wait_bytes(rs_in, rs_recv.at[k])
        for place in range(4):
            image = image + rs_in[place].astype(jnp.float32)
        y_own[k, wi] = image
        pltpu.make_async_remote_copy(
            src_ref=y_own.at[k, wi], dst_ref=y_own.at[k, wi],
            send_sem=own_send.at[k], recv_sem=own_recv.at[k],
            device_id={"wa": other}, device_id_type=MESH,
        ).start()
        if k < ITERS:
            rounded = image.astype(jnp.bfloat16)
            y[k, mine] = rounded
            y[k, own_column] = rounded
            gather_start(2 + k, y.at[k, mine], y.at[k])
            forward(2 + k, y.at[k, mine], y.at[k], mine, 0)
            share_sums()
            column_start(2 + k, y.at[k, mine], y.at[k])
        wait_bytes(rs_out, rs_send.at[k])
        wait_bytes(relay_out, relay_send.at[k])
        if k == 0:
            gather_finish(1, dl_all)
            column_finish(1, dl_all)
            rest = level_ref[...]
            found = jnp.zeros(((chunks + lb) * half, width), jnp.float32)
            for _ in range(3):
                term = rest.astype(jnp.bfloat16)
                rest = rest - term.astype(jnp.float32)
                found = found + jnp.dot(
                    dl_all[...].reshape((chunks + lb) * half, 128), term, preferred_element_type=jnp.float32
                )
            diag[...] = found.reshape(chunks + lb, half, width)
        arrivals = [0] + plane_steps
        wait_bytes(sc_z.at[k, pl.ds(0, 2 * lb - 1)], z_recv.at[k])
        total = sc_z[k, 0]
        for j in range(1, 2 * lb):
            total = total + sc_z[k, j]
        total = jnp.sum(total, axis=1, keepdims=True) * (1.0 / total_count)
        scalars = [jnp.broadcast_to(total[q : q + 1], TILE) for q in range(2 * k + 2)]
        for j in range(k + 1):
            gram[(j, k)] = gram[(k, j)] = scalars[j]
            cross[(j, k)] = cross[(k, j)] = scalars[k + 1 + j]
        raw = [jnp.zeros(TILE, jnp.float32) for _ in range(k)] + [jnp.ones(TILE, jnp.float32)]
        for j in range(k):
            correlation = sum(mix[(j, i)] * gram[(i, k)] for i in range(j + 1))
            for i in range(j + 1):
                raw[i] = raw[i] - correlation * mix[(j, i)]
        norm = jnp.zeros(TILE, jnp.float32)
        for i in range(k + 1):
            norm = norm + raw[i] * sum(raw[j] * gram[(i, j)] for j in range(k + 1))
        scale = lax.rsqrt(jnp.maximum(norm, 0.0) + epsilon)
        for i in range(k + 1):
            mix[(k, i)] = raw[i] * scale
        entries = {}
        for b in range(k + 1):
            image_row = [
                sum(mix[(b, j)] * cross[(i, j)] for j in range(b + 1)) for i in range(b + 1)
            ]
            for a in range(b + 1):
                entries[(a, b)] = sum(mix[(a, i)] * image_row[i] for i in range(a + 1))
        theta, weights = lowest(entries, k + 1)
        alphas = [
            sum(weights[j] * mix[(j, i)] for j in range(i, k + 1)) for i in range(k + 1)
        ]
        for i in range(k + 1):
            coef[i] = alphas[i]
            coef[4 + i] = -(theta * alphas[i])
        coef[8] = theta

        if k < ITERS:

            def correct_late(index, carry):
                step = pick(arrivals, index)
                slot = source_of(step) * 2 + wi
                wait_bytes(y.at[k, slot], gather_recv.at[2 + k, step])
                forward(2 + k, y.at[k, slot], y.at[k], slot, step)
                return correct(k, slot, carry)

            def correct_other(index, carry):
                step = pick(arrivals, index)
                slot = source_of(step) * 2 + other
                wait_bytes(y.at[k, slot], fwd_recv.at[2 + k, step])
                return correct(k, slot, carry)

            correct(k, mine, 0)
            lax.fori_loop(1, rb, correct_late, 0)
            lax.fori_loop(0, rb, correct_other, 0)

    for k in range(ITERS + 1):
        wait_bytes(y_own.at[k, other], own_recv.at[k])
    theta_rows = tiled(coef[8], half, width)
    for h in range(2):
        ritz_rows = jnp.zeros((half, width), jnp.float32)
        image_rows = jnp.zeros((half, width), jnp.float32)
        for i in range(ITERS + 1):
            alpha = tiled(coef[i], half, width)
            ritz_rows = ritz_rows + alpha * x[i, ri * 2 + h].astype(jnp.float32)
            image_rows = image_rows + alpha * y_own[i, h]
        image_rows = image_rows - theta_rows * ritz_rows
        for s in range(physical):
            ritz_ref[h * half : (h + 1) * half, s, :] = ritz_rows[:, s * window : (s + 1) * window]
            residual_ref[h * half : (h + 1) * half, s, :] = image_rows[:, s * window : (s + 1) * window]
    gather_drain(0, x.at[0], rb - 1)
    gather_drain(1, dl_all, rb - 1)
    for k in range(ITERS):
        gather_drain(2 + k, y.at[k], rb)
    wait_bytes(sc_xy.at[0, pl.ds(0, rb - 1)], xy_send.at[0])
    for k in range(1, ITERS + 1):
        wait_bytes(sc_xy.at[k, pl.ds(0, rb - 1)], xy_send.at[k])
    for k in range(ITERS + 1):
        wait_bytes(sc_z.at[k, pl.ds(0, 2 * lb - 1)], z_send.at[k])
        wait_bytes(y_own.at[k, wi], own_send.at[k])


def copy_kernel(first_in, second_in, first_out, second_out):
    first_out[...] = first_in[...]
    second_out[...] = second_in[...]


def per_device(initial_guess, left_environment, right_environment, operator_blocks, operator_pairs):
    own, physical, window = initial_guess.shape
    width = physical * window
    levels = right_environment.shape[1]
    local_levels, lb, _, _, depth = left_environment.shape
    rb, wa = lax.axis_size("rb"), lax.axis_size("wa")
    half = own // wa
    side = 1
    while side * side < rb:
        side += 1
    left = left_environment.reshape(local_levels, lb, own, depth)
    sizes = (lb, rb, wa, side, half, width, window, levels, own * lb * rb * width)
    f32, bf16 = jnp.float32, jnp.bfloat16
    DMA = pltpu.SemaphoreType.DMA
    n = ITERS + 1
    vmem = pl.BlockSpec(memory_space=pltpu.VMEM)
    smem = pl.BlockSpec(memory_space=pltpu.SMEM)
    blocks = operator_blocks.shape[0]
    pairs_of_states = physical * (physical + 1) // 2
    ritz, residual = pl.pallas_call(
        functools.partial(davidson_kernel, sizes),
        out_shape=[jax.ShapeDtypeStruct((own, physical, window), f32)] * 2,
        in_specs=[vmem, pl.BlockSpec(memory_space=pl.ANY), vmem, smem, smem],
        out_specs=[vmem, vmem],
        scratch_shapes=[
            pltpu.VMEM((local_levels * width, width), bf16),
            pltpu.VMEM((128, width), f32),
            pltpu.VMEM((window, levels, window), f32),
            pltpu.VMEM((levels, window, window), f32),
            pltpu.VMEM((levels, window), f32),
            pltpu.SMEM((blocks, pairs_of_states), f32),
            pltpu.VMEM((own, physical, window), f32),
            pltpu.VMEM((local_levels, len(FAR), own, depth), bf16),
            pltpu.VMEM((local_levels, len(NEAR), own, depth), bf16),
            pltpu.VMEM((n, 2 * rb + lb, half, width), bf16),
            pltpu.VMEM((ITERS, 2 * rb + lb, half, width), bf16),
            pltpu.VMEM((n, 2, half, width), f32),
            pltpu.VMEM((len(FAR) * own, local_levels * width), bf16),
            pltpu.VMEM((len(NEAR) * own, local_levels * width), bf16),
            pltpu.VMEM((len(FAR), 2, half, width), f32),
            pltpu.VMEM((len(NEAR), 2, half, width), f32),
            pltpu.VMEM((len(FAR), half, width), bf16),
            pltpu.VMEM((len(FAR), half, width), bf16),
            pltpu.VMEM((len(NEAR), half, width), bf16),
            pltpu.VMEM((len(NEAR), half, width), bf16),
            pltpu.VMEM((len(FAR), half, width), bf16),
            pltpu.VMEM((2, half, width), bf16),
            pltpu.VMEM((2, half // 2, width), bf16),
            pltpu.VMEM((4, half, width), bf16),
            pltpu.VMEM((4, half, width), bf16),
            pltpu.VMEM((own, 128), bf16),
            pltpu.VMEM((own, 128), bf16),
            pltpu.VMEM((2 * rb + lb, half, 128), bf16),
            pltpu.VMEM((2 * rb + lb, half, width), f32),
            pltpu.VMEM((9,) + TILE, f32),
            pltpu.VMEM((n, rb) + TILE, f32),
            pltpu.VMEM((n, 2 * lb) + TILE, f32),
            DMA((lb,)),
            DMA((2 + ITERS,)),
            DMA((2 + ITERS, rb)),
            DMA((2 + ITERS,)),
            DMA((2 + ITERS, rb)),
            DMA((2 + ITERS,)),
            DMA((2 + ITERS,)),
            DMA((n,)),
            DMA((n,)),
            DMA((n,)),
            DMA((n,)),
            DMA((n, 2)),
            DMA((n, 2)),
            DMA((n,)),
            DMA((n,)),
            DMA((n,)),
            DMA((n,)),
            DMA((n,)),
            DMA((n,)),
            DMA((n,)),
            DMA((2,)),
        ],
        compiler_params=pltpu.CompilerParams(
            collective_id=0, has_side_effects=True, vmem_limit_bytes=60 * 1024 * 1024
        ),
    )(
        initial_guess, left, right_environment,
        jnp.transpose(operator_blocks, (1, 2, 0)), jnp.transpose(operator_pairs),
    )
    return pl.pallas_call(
        copy_kernel,
        out_shape=[jax.ShapeDtypeStruct((own, physical, window), f32)] * 2,
        in_specs=[vmem, vmem],
        out_specs=[vmem, vmem],
    )(ritz, residual)


def solution(mesh):
    in_specs = (P(("lb", "rb"), None, None), P("wa", None, "rb", None, "lb"), P(), P(), P())
    out_specs = (P(("lb", "rb"), None, None), P(("lb", "rb"), None, None))
    return jax.shard_map(
        per_device, mesh=mesh, in_specs=in_specs, out_specs=out_specs, check_vma=False
    )
```
